32 devices in a mesh: row: 8 (over y, x, core), col: 4 (over z).
Axes of the slice: x: 2, y: 2, z: 4, core: 2. Of those that a mesh axis runs over, the one named last changes fastest.
Arguments:
- velocity: float32 [3, 2, 128, 256, 256], P(None, None, 'row', 'col'), may hold values from -7.5 to 7.5
- accumulator: float32 [3, 2, 128, 256, 256], P(None, None, 'row', 'col'), may hold values from -6 to 6
- remesh_flag: int32 [128], P('row'), may hold values 0 or 1
- remesh_shift: int32 [128], P('row'), may hold values from -128 to 127
- viscosity: float32 [1], replicated, may hold values from 0.0003 to 0.0015
- shear: float32 [1], replicated, may hold values from 8 to 20
- clock: float32 [1], replicated, may hold values from 0 to 0.05
- step: float32 [1], replicated, may hold values from 0.004 to 0.01
Outputs:
- new_velocity: float32 [3, 2, 128, 256, 256], P(None, None, 'row', 'col')
- new_accumulator: float32 [3, 2, 128, 256, 256], P(None, None, 'row', 'col')
- spectra: float32 [2, 128], P(None, 'row')
The draws below stay inside these ranges and needn't reach their ends.
All inputs are finite; a program needn't handle non-finite values. No bound on the sum of `remesh_flag` on one device may be relied on, other than what follows from the above.
Results may differ from the reference program's by a relative error of at most 0.0001.
Values sent between devices are 32-bit elements; how exact they have to be, the bound alone decides.
A program may use at most 192 MiB of HBM per device.

```python
import math
import jax
import jax.numpy as jnp

NX = 256
NY = 256
NZ = 256
KX = 128


def draw_velocity(key, part):
    first_key = jax.random.fold_in(jax.random.fold_in(key, 11), 0)
    sample = jnp.clip(jax.random.normal(first_key, (3, 2, KX, NZ, NY), jnp.float32), -4.0, 4.0)
    correlated = sample.at[1].add(-0.6 * sample[0])
    return correlated


def set_ends(entries, stream_key, smallest, top_value):
    shape = entries.shape
    spot = [jax.random.randint(jax.random.fold_in(stream_key, axis), (), 0, shape[axis]) for axis in range(len(shape))]
    entries = entries.at[tuple(spot)].set(smallest)
    longest = shape.index(max(shape))
    spot[longest] = (spot[longest] + 1) % shape[longest]
    return entries.at[tuple(spot)].set(top_value)


def block_levels(stream_key, extent, cuts, low, high):
    gain = 1.0
    for position, parts in cuts:
        heights = jax.random.uniform(jax.random.fold_in(jax.random.fold_in(stream_key, 6), position), (parts,), jnp.float32, low / len(cuts), high / len(cuts))
        gain = gain * jnp.repeat(jnp.exp(heights), extent[position] // parts).reshape((-1,) + (1,) * (len(extent) - 1 - position))
    return gain


def gaussian(key, shape, width, bound, cuts=(), held_as=jnp.bfloat16):
    values = width * jax.random.normal(key, shape, jnp.float32)
    if cuts:
        values = values * block_levels(key, shape, cuts, -0.22, 0.18)
    return jnp.clip(values, -bound, bound).astype(held_as)


def setup_inputs(seed: int = 0) -> dict:
    key_list = jax.random.split(jax.random.key(seed), 9)
    return {
        "velocity": draw_velocity(jax.random.fold_in(key_list[8], 71), 0),
        "accumulator": gaussian(key_list[1], (3, 2, KX, NZ, NY), 1.0, 6.0, ((2, 8), (3, 4)), jnp.float32),
        "remesh_flag": set_ends((jax.random.randint(key_list[2], (KX,), 0, 2) < 1).astype(jnp.int32), jax.random.fold_in(key_list[2], 1), 0, 1),
        "remesh_shift": set_ends(jax.random.randint(key_list[3], (KX,), 0 - NY // 2, NY // 2), jax.random.fold_in(key_list[3], 1), 0 - NY // 2, (NY // 2) - 1).astype(jnp.int32),
        "viscosity": jnp.clip(jnp.exp(jax.random.uniform(key_list[4], (1,), jnp.float32, math.log(0.0003), math.log(0.0015))), 0.0003, 0.0015),
        "shear": jnp.clip(jax.random.uniform(key_list[5], (1,), jnp.float32, 8.0, 20.0), 8.0, 20.0),
        "clock": jnp.clip(jax.random.uniform(key_list[6], (1,), jnp.float32, 0.0, 0.05), 0.0, 0.05),
        "step": jnp.clip(jax.random.uniform(key_list[7], (1,), jnp.float32, 0.004, 0.01), 0.004, 0.01),
    }


def signed_index(positions, period):
    return jnp.where(2 * positions < period, positions, positions - period)


def roll_rows(field, amounts):
    def shift_row(row_data, amount_one):
        return jnp.roll(row_data, -amount_one, axis=-1)
    return jax.vmap(shift_row, in_axes=(2, 0), out_axes=2)(field, amounts)


def project(real_part, imag_part, wave_vector, inverse_square):
    along_real = (wave_vector[0] * real_part[0] + wave_vector[1] * real_part[1] + wave_vector[2] * real_part[2]) * inverse_square
    along_imag = (wave_vector[0] * imag_part[0] + wave_vector[1] * imag_part[1] + wave_vector[2] * imag_part[2]) * inverse_square
    return (jnp.stack([real_part[number] - wave_vector[number] * along_real for number in range(3)]),
            jnp.stack([imag_part[number] - wave_vector[number] * along_imag for number in range(3)]))


def cross_product(first_one, second_one):
    return jnp.stack([first_one[1] * second_one[2] - first_one[2] * second_one[1],
                      first_one[2] * second_one[0] - first_one[0] * second_one[2],
                      first_one[0] * second_one[1] - first_one[1] * second_one[0]])


def to_grid(real_part, imag_part):
    weights = jnp.where(jnp.arange(KX) == 0, 1.0, 2.0).astype(jnp.float32)[:, None, None]
    result_list = []
    for number in range(3):
        half = weights * (real_part[number] + 1j * imag_part[number])
        full = jnp.zeros((NX, NZ, NY), half.dtype).at[:KX].set(half)
        result_list.append(jnp.real(jnp.fft.ifftn(full, norm="ortho")))
    return jnp.stack(result_list)


def reference(velocity, accumulator, remesh_flag, remesh_shift, viscosity, shear, clock, step):
    offset = remesh_flag * remesh_shift
    remeshed = roll_rows(velocity, offset)
    carried = roll_rows(accumulator, offset)
    lattice_x = jnp.arange(KX, dtype=jnp.int32)
    lattice_z = signed_index(jnp.arange(NZ, dtype=jnp.int32), NZ)
    lattice_y = signed_index(jnp.arange(NY, dtype=jnp.int32), NY)
    wave_x = lattice_x.astype(jnp.float32)[:, None, None]
    wave_z = lattice_z.astype(jnp.float32)[None, :, None]
    wave_y = lattice_y.astype(jnp.float32)[None, None, :] - shear[0] * clock[0] * wave_x
    wave_vector = (wave_x, wave_y, wave_z)
    square_wave = wave_x * wave_x + wave_y * wave_y + wave_z * wave_z
    inverse_square = 1.0 / jnp.maximum(square_wave, 1.0)
    dealias_mask = ((3 * lattice_x < NX)[:, None, None] & (3 * jnp.abs(lattice_z) < NZ)[None, :, None]
                    & (3 * jnp.abs(lattice_y) < NY)[None, None, :]).astype(jnp.float32)
    solen_real, solen_imag = project(remeshed[:, 0], remeshed[:, 1], wave_vector, inverse_square)
    smooth_real = dealias_mask * solen_real
    smooth_imag = dealias_mask * solen_imag
    vort_real = -cross_product(wave_vector, smooth_imag)
    vort_imag = cross_product(wave_vector, smooth_real)
    flow_grid = to_grid(smooth_real, smooth_imag)
    swirl_grid = to_grid(vort_real, vort_imag)
    lamb_grid = cross_product(flow_grid, swirl_grid)
    lamb_hat = [jnp.fft.fftn(lamb_grid[number], norm="ortho")[:KX] for number in range(3)]
    hat_real = dealias_mask * jnp.stack([jnp.real(spectrum) for spectrum in lamb_hat])
    hat_imag = dealias_mask * jnp.stack([jnp.imag(spectrum) for spectrum in lamb_hat])
    proj_real, proj_imag = project(hat_real, hat_imag, wave_vector, inverse_square)
    shear_rate = shear[0]
    viscous_rate = viscosity[0]
    coupling = 2.0 * shear_rate * wave_x * inverse_square

    def tendency(projected, state):
        term_list = [projected[number] + coupling * wave_vector[number] * state[1] - viscous_rate * square_wave * state[number] for number in range(3)]
        term_list[0] = term_list[0] - shear_rate * state[1]
        return jnp.stack(term_list)

    tendencies = jnp.stack([tendency(proj_real, remeshed[:, 0]), tendency(proj_imag, remeshed[:, 1])], axis=1)
    new_accumulator = (-5.0 / 9.0) * carried + step[0] * tendencies
    new_velocity = remeshed + (15.0 / 16.0) * new_accumulator
    stress = jnp.sum(remeshed[0, 0] * remeshed[1, 0] + remeshed[0, 1] * remeshed[1, 1], axis=(1, 2)) / (NY * NZ)
    energy = jnp.sum(remeshed * remeshed, axis=(0, 1))
    dissipation = 2.0 * viscous_rate * jnp.sum(square_wave * energy, axis=(1, 2)) / (NY * NZ)
    return new_velocity, new_accumulator, jnp.stack([stress, dissipation])
```

```python
import functools

import jax
import jax.numpy as jnp
import ml_dtypes
import numpy as np
from jax import lax
from jax.experimental import pallas as pl
from jax.experimental.pallas import tpu as pltpu
from jax.sharding import PartitionSpec as P

NX = 256
NY = 256
NZ = 256
LAG = 2
OCT = 8
VMEM_BYTES = 60 * 1024 * 1024
F32 = jnp.float32
BF16 = jnp.bfloat16


def tables(period):
    positions = np.arange(period)
    angles = (positions[:, None] * positions[None, :] % period) * (2.0 * np.pi / period)
    factor = 1.0 / np.sqrt(period)
    return np.cos(angles) * factor, np.sin(angles) * factor


def halves(table):
    table = np.ascontiguousarray(table).astype(np.float32)
    high = table.astype(ml_dtypes.bfloat16)
    low = (table - high.astype(np.float32)).astype(ml_dtypes.bfloat16)
    return [jnp.asarray(high), jnp.asarray(low)]


class Plan:
    def __init__(self, rows, cols, width_x, width_z):
        self.rows, self.cols = rows, cols
        self.wx, self.wz = width_x, width_z
        self.by, self.bz = NY // cols, NZ // rows
        self.live = sum(1 for k in range(rows * width_x) if 3 * k < NX)
        self.slots = -(-self.live // OCT) * OCT
        self.nh = width_x // OCT
        self.octs = self.slots // OCT
        alive = [3 * min(k, NZ - k) < NZ for k in range(NZ)]
        self.window = []
        self.offset = []
        total = 0
        for h in range(cols):
            inside = [k for k in range(width_z) if alive[h * width_z + k]]
            low = inside[0] // 8 * 8 if inside else 0
            high = -(-(inside[-1] + 1) // 8) * 8 if inside else 0
            self.window.append((low, high - low))
            self.offset.append(total)
            total += high - low
        self.kz = [
            h * width_z + low + k for h, (low, n) in enumerate(self.window) for k in range(n)
        ]
        self.stride = self.bz + 8 if self.bz % 16 == 0 else self.bz
        self.zg = max(1, min(self.bz, 256 // self.by))


def make_tables(plan):
    cos_x, sin_x = tables(NX)
    cos_y, sin_y = tables(NY)
    cos_z, sin_z = tables(NZ)
    cy = cos_y.reshape(NY, plan.cols, plan.by)
    sy = sin_y.reshape(NY, plan.cols, plan.by)
    inv_y = np.concatenate(
        [np.concatenate([cy, sy], 2), np.concatenate([-sy, cy], 2)], 0
    ).reshape(2 * NY, 2 * NY)
    inv_zc, inv_zs = cos_z[:, plan.kz], sin_z[:, plan.kz]
    kx = np.arange(plan.slots)
    weight = np.where(kx == 0, 1.0, 2.0) * (kx < plan.live)
    cx, sx = cos_x[:, : plan.slots], sin_x[:, : plan.slots]
    inv_x = np.concatenate([cx * weight, -sx * weight], 1)
    keep = (kx < plan.live)[:, None]
    fwd_x = np.concatenate([cx.T * keep, -sx.T * keep], 0)
    cy = cos_y.reshape(plan.cols, plan.by, NY)
    sy = sin_y.reshape(plan.cols, plan.by, NY)
    fwd_y = np.concatenate(
        [np.concatenate([cy, -sy], 2), np.concatenate([sy, cy], 2)], 1
    ).reshape(2 * NY, 2 * NY)
    return {
        "inv_y": halves(inv_y),
        "inv_z": halves(inv_zc) + halves(inv_zs),
        "inv_x": halves(inv_x),
        "fwd_x": halves(fwd_x),
        "fwd_z": halves(inv_zc.T) + halves(inv_zs.T),
        "fwd_y": halves(fwd_y),
    }


def split(value):
    high = value.astype(BF16)
    return high, (value - high.astype(F32)).astype(BF16)


def mul(a, b):
    return jnp.dot(a, b, preferred_element_type=F32)


def dot3(ah, al, bh, bl):
    return mul(ah, bh) + mul(ah, bl) + mul(al, bh)


def geometry(kx, first_z, real, shape):
    iz = lax.broadcasted_iota(jnp.int32, shape, 0) + first_z
    iz = jnp.where(2 * iz < NZ, iz, iz - NZ)
    iy = lax.broadcasted_iota(jnp.int32, shape, 1)
    iy = jnp.where(2 * iy < NY, iy, iy - NY)
    k0 = jnp.full(shape, kx.astype(F32), F32)
    k1 = iy.astype(F32) - real[4] * k0
    k2 = iz.astype(F32)
    ksq = k0 * k0 + k1 * k1 + k2 * k2
    inv = 1.0 / jnp.maximum(ksq, 1.0)
    keep = (3 * jnp.abs(iz) < NZ) & (3 * jnp.abs(iy) < NY) & (3.0 * k0 < float(NX))
    return (k0, k1, k2), ksq, inv, keep


def project(field, k, inv):
    along = (k[0] * field[0] + k[1] * field[1] + k[2] * field[2]) * inv
    return [field[c] - k[c] * along for c in range(3)]


def greet(rows, cols):
    row, col = lax.axis_index("row"), lax.axis_index("col")
    barrier = pltpu.get_barrier_semaphore()
    for k in range(1, cols):
        pl.semaphore_signal(
            barrier, inc=1, device_id={"col": (col + k) % cols},
            device_id_type=pl.DeviceIdType.MESH,
        )
    for k in range(1, rows):
        pl.semaphore_signal(
            barrier, inc=1, device_id={"row": (row + k) % rows},
            device_id_type=pl.DeviceIdType.MESH,
        )
    pl.semaphore_wait(barrier, rows + cols - 2)


def remote(src, dst, send, recv, axis, index):
    return pltpu.make_async_remote_copy(
        src_ref=src, dst_ref=dst, send_sem=send, recv_sem=recv,
        device_id={axis: index}, device_id_type=pl.DeviceIdType.MESH,
    )


def backward_part(
    plan, grid_in, ixh, ixl, fxh, fxl, ch, cl, sh, sl,
    modes, blocks, spans, lines, row_send, row_recv, col_send, col_recv,
):
    row, col = lax.axis_index("row"), lax.axis_index("col")
    rows, cols, by, bz, zg = plan.rows, plan.cols, plan.by, plan.bz, plan.zg
    slots, octs, nh = plan.slots, plan.octs, plan.nh
    chunks = nh * 5

    def grid_step(g, carry):
        fields = []
        for c in range(3):
            lines_z = [
                grid_in[c, pl.ds(g * zg + z, slots, stride=plan.stride), :]
                for z in range(zg)
            ]
            packed = jnp.concatenate(
                [
                    jnp.concatenate([f[:, :by] for f in lines_z], 1),
                    jnp.concatenate([f[:, by:] for f in lines_z], 1),
                ],
                0,
            )
            high, low = split(packed)
            fields.append(dot3(ixh[...], ixl[...], high, low))
        u, v, w = fields
        ww = w * w
        for p, product in enumerate((u * u - ww, v * v - ww, u * v, u * w, v * w)):
            high, low = split(product)
            made = dot3(fxh[...], fxl[...], high, low)
            for z in range(zg):
                line = jnp.concatenate(
                    [
                        made[:slots, z * by : (z + 1) * by],
                        made[slots:, z * by : (z + 1) * by],
                    ],
                    1,
                )
                for o in range(octs):
                    blocks[
                        p, o, pl.ds(pl.multiple_of((g * zg + z) * OCT, OCT), OCT), :
                    ] = line[o * OCT : (o + 1) * OCT]
        return carry

    lax.fori_loop(0, bz // zg, grid_step, 0)

    def row_copy(c, o, s, source):
        return remote(
            blocks.at[c % 5, o],
            spans.at[c, pl.ds(source * bz * OCT, bz * OCT), :],
            row_send.at[c, s], row_recv.at[c, source], "row", s,
        )

    def live(s, c):
        return s * nh + c // 5 < octs

    def send(c, carry):
        for j in range(1, rows):
            s = (row + j) % rows

            @pl.when(live(s, c))
            def _():
                row_copy(c, s * nh + c // 5, s, row).start()

        return carry

    lax.fori_loop(0, chunks, send, 0)

    def col_copy(c, q, source):
        low, n = plan.window[q]
        off = plan.offset[q]
        return remote(
            lines.at[c, :, pl.ds(off, n), :],
            modes.at[c, source, :, pl.ds(low, n), :],
            col_send.at[c, q], col_recv.at[c, source], "col", q,
        )

    def keep_copy(c, q):
        low, n = plan.window[q]
        off = plan.offset[q]
        return pltpu.make_async_copy(
            lines.at[c, :, pl.ds(off, n), :],
            modes.at[c, col, :, pl.ds(low, n), :],
            col_send.at[c, q],
        )

    def span_step(c, carry):
        @pl.when(live(row, c))
        def _():
            spans[c, pl.ds(pl.multiple_of(row * bz * OCT, OCT), bz * OCT), :] = blocks[
                c % 5, row * nh + c // 5
            ]
            for j in range(1, rows):
                row_copy(c, 0, row, (row + j) % rows).wait_recv()
            for k in range(0, OCT, 2):
                x = [
                    spans[c, pl.ds(k + m, NZ, stride=OCT), :] for m in range(2)
                ]
                turned = [jnp.concatenate([f[:, by:], -f[:, :by]], 1) for f in x]
                xh, xl = split(jnp.concatenate(x, 1))
                th, tl = split(jnp.concatenate(turned, 1))
                made = dot3(ch[...], cl[...], xh, xl) + dot3(sh[...], sl[...], th, tl)
                for m in range(2):
                    lines[c, k + m] = made[:, m * 2 * by : (m + 1) * 2 * by]
            for j in range(1, cols):
                for q in range(cols):
                    if plan.window[q][1]:

                        @pl.when((col + j) % cols == q)
                        def _():
                            col_copy(c, q, col).start()

            for q in range(cols):
                if plan.window[q][1]:

                    @pl.when(col == q)
                    def _():
                        keep_copy(c, q).start()

        return carry

    lax.fori_loop(0, chunks, span_step, 0)

    def drain(c, carry):
        for j in range(1, rows):
            s = (row + j) % rows

            @pl.when(live(s, c))
            def _():
                row_copy(c, s * nh + c // 5, s, row).wait_send()

        @pl.when(live(row, c))
        def _():
            for q in range(cols):
                if plan.window[q][1]:

                    @pl.when(col == q)
                    def _():
                        keep_copy(c, q).wait()
                        for j in range(1, cols):
                            col_copy(c, q, (q + j) % cols).wait_recv()

                    @pl.when(col != q)
                    def _():
                        col_copy(c, q, col).wait_send()

        return carry

    lax.fori_loop(0, chunks, drain, 0)


def middle_kernel(
    plan, amount, real, vel, yh, yl, ch, cl, sh, sl,
    ixh, ixl, fxh, fxl, bch, bcl, bsh, bsl,
    modes, sums, grid_in, part, lines, spans, own, parts,
    col_send, col_recv, row_send, row_recv, sum_send, sum_recv, *back,
):
    step = pl.program_id(0)
    row, col = lax.axis_index("row"), lax.axis_index("col")
    rows, cols, wx, wz, by, bz = plan.rows, plan.cols, plan.wx, plan.wz, plan.by, plan.bz
    shape = (wz, NY)

    @pl.when(step == 0)
    def _():
        for c in range(3):
            for s in range(plan.live, plan.slots):
                grid_in[c, s * plan.stride : s * plan.stride + bz] = jnp.zeros(
                    (bz, 2 * by), F32
                )
        greet(rows, cols)

    def col_copy(i, h, q):
        low, n = plan.window[h]
        off = plan.offset[h]
        return remote(
            part.at[i, q, :, pl.ds(low, n), :], lines.at[i, :, pl.ds(off, n), :],
            col_send.at[i, q], col_recv.at[i, h], "col", q,
        )

    def row_copy(i, slot, r):
        return remote(
            spans.at[i, :, pl.ds(r * bz, bz), :],
            grid_in.at[:, pl.ds(slot * plan.stride, bz), :],
            row_send.at[i, r], row_recv.at[slot], "row", r,
        )

    def sum_copy(q):
        return remote(own, parts.at[col], sum_send.at[q], sum_recv.at[col], "col", q)

    @pl.when(step < wx)
    def _():
        i = step
        kx = row * wx + i
        k, ksq, inv, keep = geometry(kx, col * wz, real, shape)
        shift = amount[i]
        v = [[pltpu.roll(vel[c, p, 0], shift, 1) for p in range(2)] for c in range(3)]
        stress = v[0][0] * v[1][0] + v[0][1] * v[1][1]
        energy = sum(v[c][p] * v[c][p] for c in range(3) for p in range(2))
        own[i, 0:1] = jnp.sum(stress, axis=0, keepdims=True)
        own[i, 1:2] = jnp.sum(ksq * energy, axis=0, keepdims=True)

        @pl.when(kx < plan.live)
        def _():
            mask = jnp.where(keep, 1.0, 0.0)
            out = [project([v[c][p] for c in range(3)], k, inv) for p in range(2)]
            smooth = jnp.concatenate(
                [
                    jnp.concatenate([mask * out[0][c], mask * out[1][c]], 1)
                    for c in range(3)
                ],
                0,
            )
            high, low = split(smooth)
            made = dot3(high, low, yh[...], yl[...])
            for q in range(cols):
                for c in range(3):
                    part[i, q, c] = made[
                        c * wz : (c + 1) * wz, q * 2 * by : (q + 1) * 2 * by
                    ]
            for h in range(cols):
                if plan.window[h][1]:
                    low, n = plan.window[h]
                    off = plan.offset[h]

                    @pl.when(col == h)
                    def _():
                        lines[i, :, off : off + n, :] = part[i, h, :, low : low + n, :]
                        for j in range(1, cols):
                            q = (h + j) % cols
                            col_copy(i, h, q).start()

    @pl.when(step == wx)
    def _():
        for j in range(1, cols):
            sum_copy((col + j) % cols).start()

    @pl.when(step >= LAG)
    def _():
        i = step - LAG
        kx = row * wx + i

        @pl.when(kx < plan.live)
        def _():
            for h in range(cols):
                if plan.window[h][1]:

                    @pl.when(col != h)
                    def _():
                        col_copy(i, h, col).wait_recv()

            x = [lines[i, c] for c in range(3)]
            turned = [jnp.concatenate([-f[:, by:], f[:, :by]], 1) for f in x]
            xh, xl = split(jnp.concatenate(x, 1))
            th, tl = split(jnp.concatenate(turned, 1))
            made = dot3(ch[...], cl[...], xh, xl) + dot3(sh[...], sl[...], th, tl)
            for c in range(3):
                spans[i, c] = made[:, c * 2 * by : (c + 1) * 2 * by]
            for r in range(rows):

                @pl.when(row == r)
                def _():
                    for c in range(3):
                        grid_in[c, pl.ds(pl.multiple_of(kx * plan.stride, 8), bz)] = spans[
                            i, c, r * bz : (r + 1) * bz
                        ]

            for j in range(1, rows):
                row_copy(i, kx, (row + j) % rows).start()

    @pl.when(step == wx + LAG - 1)
    def _():
        def arrived(slot, carry):
            @pl.when(slot // wx != row)
            def _():
                row_copy(0, slot, row).wait_recv()

            return carry

        lax.fori_loop(0, plan.live, arrived, 0)
        backward_part(
            plan, grid_in, ixh, ixl, fxh, fxl, bch, bcl, bsh, bsl, modes, *back
        )

        def sent(i, carry):
            @pl.when(row * wx + i < plan.live)
            def _():
                for h in range(cols):
                    if plan.window[h][1]:

                        @pl.when(col == h)
                        def _():
                            for j in range(1, cols):
                                col_copy(i, h, (h + j) % cols).wait_send()

                for j in range(1, rows):
                    row_copy(i, row * wx + i, (row + j) % rows).wait_send()

            return carry

        lax.fori_loop(0, wx, sent, 0)
        total = own[...]
        for j in range(1, cols):
            h = (col + j) % cols
            remote(
                own, parts.at[h], sum_send.at[h], sum_recv.at[h], "col", h
            ).wait()
        parts[col] = total
        sums[...] = sum(parts[h] for h in range(cols))


def last_kernel(plan, amount, base, real, vel, acc, modes, fh, fl, new_vel, new_acc, hats):
    shape = vel.shape[3:]
    kx = base[0] + pl.program_id(0)
    k, ksq, inv, keep = geometry(kx, base[1], real, shape)
    shift = amount[pl.program_id(0)]
    viscosity, shear, step = real[0], real[1], real[3]
    coupling = 2.0 * shear * k[0] * inv
    wz = shape[0]

    @pl.when(kx < plan.live)
    def _():
        packed = jnp.concatenate(
            [
                jnp.concatenate([modes[0, p, h, 0] for h in range(plan.cols)], 1)
                for p in range(5)
            ],
            0,
        )
        high, low = split(packed)
        hats[...] = dot3(high, low, fh[...], fl[...])

    for p in range(2):
        v = [pltpu.roll(vel[c, p, 0], shift, 1) for c in range(3)]
        old = [pltpu.roll(acc[c, p, 0], shift, 1) for c in range(3)]
        other = slice((1 - p) * NY, (2 - p) * NY)
        e0, e1, e01, e02, e12 = [
            jnp.where(keep, hats[m * wz : (m + 1) * wz, other], 0.0) for m in range(5)
        ]
        sign = 1.0 if p == 0 else -1.0
        hat = [
            sign * (k[0] * e0 + k[1] * e01 + k[2] * e02),
            sign * (k[0] * e01 + k[1] * e1 + k[2] * e12),
            sign * (k[0] * e02 + k[1] * e12),
        ]
        hat = project(hat, k, inv)
        for c in range(3):
            rate = hat[c] + coupling * k[c] * v[1] - viscosity * ksq * v[c]
            if c == 0:
                rate = rate - shear * v[1]
            total = (-5.0 / 9.0) * old[c] + step * rate
            new_acc[c, p, 0] = total
            new_vel[c, p, 0] = v[c] + (15.0 / 16.0) * total


def body(velocity, accumulator, remesh_flag, remesh_shift, viscosity, shear, clock, step):
    rows = lax.axis_size("row")
    cols = lax.axis_size("col")
    _, _, wx, wz, full_y = velocity.shape
    plan = Plan(rows, cols, wx, wz)
    by, bz = plan.by, plan.bz
    table = make_tables(plan)
    amount = jnp.mod(-(remesh_flag * remesh_shift), full_y).astype(jnp.int32)
    base = jnp.stack([lax.axis_index("row") * wx, lax.axis_index("col") * wz]).astype(
        jnp.int32
    )
    real = jnp.concatenate([viscosity, shear, clock, step, shear * clock])
    whole = pl.BlockSpec(memory_space=pltpu.VMEM)
    kz = len(plan.kz)
    chunks = plan.nh * 5
    dma = pltpu.SemaphoreType.DMA
    modes, sums = pl.pallas_call(
        functools.partial(middle_kernel, plan),
        grid_spec=pltpu.PrefetchScalarGridSpec(
            num_scalar_prefetch=2,
            grid=(wx + LAG,),
            in_specs=[
                pl.BlockSpec(
                    (3, 2, 1, wz, full_y),
                    lambda i, *_: (0, 0, jnp.minimum(i, wx - 1), 0, 0),
                )
            ]
            + [whole] * 14,
            out_specs=[pl.BlockSpec(memory_space=pl.ANY), whole],
            scratch_shapes=[
                pltpu.VMEM((3, plan.slots * plan.stride, 2 * by), F32),
                pltpu.VMEM((wx, cols, 3, wz, 2 * by), F32),
                pltpu.VMEM((wx, 3, kz, 2 * by), F32),
                pltpu.VMEM((wx, 3, NZ, 2 * by), F32),
                pltpu.VMEM((wx, 2, full_y), F32),
                pltpu.VMEM((cols, wx, 2, full_y), F32),
                dma((wx, cols)),
                dma((wx, cols)),
                dma((wx, rows)),
                dma((plan.live,)),
                dma((cols,)),
                dma((cols,)),
                pltpu.VMEM((5, plan.octs, bz * OCT, 2 * by), F32),
                pltpu.VMEM((chunks, NZ * OCT, 2 * by), F32),
                pltpu.VMEM((chunks, OCT, kz, 2 * by), F32),
                dma((chunks, rows)),
                dma((chunks, rows)),
                dma((chunks, cols)),
                dma((chunks, cols)),
            ],
        ),
        out_shape=[
            jax.ShapeDtypeStruct((chunks, cols, OCT, wz, 2 * by), F32),
            jax.ShapeDtypeStruct((wx, 2, full_y), F32),
        ],
        compiler_params=pltpu.CompilerParams(
            dimension_semantics=("arbitrary",), vmem_limit_bytes=VMEM_BYTES,
            collective_id=0, has_side_effects=True,
        ),
    )(
        amount, real, velocity, *table["inv_y"], *table["inv_z"],
        *table["inv_x"], *table["fwd_x"], *table["fwd_z"],
    )
    modes = modes.reshape(plan.nh, 5, cols, OCT, wz, 2 * by)
    state_spec = pl.BlockSpec((3, 2, 1, wz, full_y), lambda i, *_: (0, 0, i, 0, 0))
    new_velocity, new_accumulator = pl.pallas_call(
        functools.partial(last_kernel, plan),
        grid_spec=pltpu.PrefetchScalarGridSpec(
            num_scalar_prefetch=3,
            grid=(wx,),
            in_specs=[state_spec] * 2
            + [
                pl.BlockSpec(
                    (1, 5, cols, 1, wz, 2 * by),
                    lambda i, *_: (i // OCT, 0, 0, i % OCT, 0, 0),
                )
            ]
            + [whole] * 2,
            out_specs=[state_spec] * 2,
            scratch_shapes=[pltpu.VMEM((5 * wz, 2 * full_y), F32)],
        ),
        out_shape=[jax.ShapeDtypeStruct(velocity.shape, F32)] * 2,
        compiler_params=pltpu.CompilerParams(
            dimension_semantics=("arbitrary",), vmem_limit_bytes=48 * 1024 * 1024
        ),
    )(amount, base, real, velocity, accumulator, modes, *table["fwd_y"])
    totals = jnp.sum(sums, axis=-1)
    stress = totals[:, 0] / (NY * NZ)
    dissipation = 2.0 * viscosity[0] * totals[:, 1] / (NY * NZ)
    return new_velocity, new_accumulator, jnp.stack([stress, dissipation])


def solution(mesh):
    state = P(None, None, "row", "col", None)
    in_specs = (state, state, P("row"), P("row"), P(), P(), P(), P())
    out_specs = (state, state, P(None, "row"))
    return jax.shard_map(
        body, mesh=mesh, in_specs=in_specs, out_specs=out_specs, check_vma=False
    )
```

```python
import functools

import jax
import jax.numpy as jnp
import ml_dtypes
import numpy as np
from jax import lax
from jax.experimental import pallas as pl
from jax.experimental.pallas import tpu as pltpu
from jax.sharding import PartitionSpec as P

NX = 256
NY = 256
NZ = 256
LAG = 2
AHEAD = 1
OCT = 8
VMEM_BYTES = 60 * 1024 * 1024
F32 = jnp.float32
BF16 = jnp.bfloat16


def tables(period):
    positions = np.arange(period)
    angles = (positions[:, None] * positions[None, :] % period) * (2.0 * np.pi / period)
    factor = 1.0 / np.sqrt(period)
    return np.cos(angles) * factor, np.sin(angles) * factor


def halves(table):
    table = np.ascontiguousarray(table).astype(np.float32)
    high = table.astype(ml_dtypes.bfloat16)
    low = (table - high.astype(np.float32)).astype(ml_dtypes.bfloat16)
    return [jnp.asarray(high), jnp.asarray(low)]


class Plan:
    def __init__(self, rows, cols, width_x, width_z):
        self.rows, self.cols = rows, cols
        self.wx, self.wz = width_x, width_z
        self.by, self.bz = NY // cols, NZ // rows
        self.live = sum(1 for k in range(rows * width_x) if 3 * k < NX)
        self.slots = -(-self.live // OCT) * OCT
        self.nh = width_x // OCT
        self.octs = self.slots // OCT
        alive = [3 * min(k, NZ - k) < NZ for k in range(NZ)]
        self.window = []
        self.offset = []
        total = 0
        for h in range(cols):
            inside = [k for k in range(width_z) if alive[h * width_z + k]]
            low = inside[0] // 8 * 8 if inside else 0
            high = -(-(inside[-1] + 1) // 8) * 8 if inside else 0
            self.window.append((low, high - low))
            self.offset.append(total)
            total += high - low
        self.kz = [
            h * width_z + low + k for h, (low, n) in enumerate(self.window) for k in range(n)
        ]
        self.stride = self.bz + 8 if self.bz % 16 == 0 else self.bz
        self.zg = max(1, min(self.bz, 256 // self.by))


def make_tables(plan):
    cos_x, sin_x = tables(NX)
    cos_y, sin_y = tables(NY)
    cos_z, sin_z = tables(NZ)
    cy = cos_y.reshape(NY, plan.cols, plan.by)
    sy = sin_y.reshape(NY, plan.cols, plan.by)
    inv_y = np.concatenate(
        [np.concatenate([cy, sy], 2), np.concatenate([-sy, cy], 2)], 0
    ).reshape(2 * NY, 2 * NY)
    inv_zc, inv_zs = cos_z[:, plan.kz], sin_z[:, plan.kz]
    kx = np.arange(plan.slots)
    weight = np.where(kx == 0, 1.0, 2.0) * (kx < plan.live)
    cx, sx = cos_x[:, : plan.slots], sin_x[:, : plan.slots]
    inv_x = np.concatenate([cx * weight, -sx * weight], 1)
    keep = (kx < plan.live)[:, None]
    fwd_x = np.concatenate([cx.T * keep, -sx.T * keep], 0)
    cy = cos_y.reshape(plan.cols, plan.by, NY)
    sy = sin_y.reshape(plan.cols, plan.by, NY)
    fwd_y = np.concatenate(
        [np.concatenate([cy, -sy], 2), np.concatenate([sy, cy], 2)], 1
    ).reshape(2 * NY, 2 * NY)
    return {
        "inv_y": halves(inv_y),
        "inv_z": halves(inv_zc) + halves(inv_zs),
        "inv_x": halves(inv_x),
        "fwd_x": halves(fwd_x),
        "fwd_z": halves(inv_zc.T) + halves(inv_zs.T),
        "fwd_y": halves(fwd_y),
    }


def split(value):
    high = value.astype(BF16)
    return high, (value - high.astype(F32)).astype(BF16)


def mul(a, b):
    return jnp.dot(a, b, preferred_element_type=F32)


def dot3(ah, al, bh, bl):
    return mul(ah, bh) + mul(ah, bl) + mul(al, bh)


def geometry(kx, first_z, real, shape):
    iz = lax.broadcasted_iota(jnp.int32, shape, 0) + first_z
    iz = jnp.where(2 * iz < NZ, iz, iz - NZ)
    iy = lax.broadcasted_iota(jnp.int32, shape, 1)
    iy = jnp.where(2 * iy < NY, iy, iy - NY)
    k0 = jnp.full(shape, kx.astype(F32), F32)
    k1 = iy.astype(F32) - real[4] * k0
    k2 = iz.astype(F32)
    ksq = k0 * k0 + k1 * k1 + k2 * k2
    inv = 1.0 / jnp.maximum(ksq, 1.0)
    keep = (3 * jnp.abs(iz) < NZ) & (3 * jnp.abs(iy) < NY) & (3.0 * k0 < float(NX))
    return (k0, k1, k2), ksq, inv, keep


def project(field, k, inv):
    along = (k[0] * field[0] + k[1] * field[1] + k[2] * field[2]) * inv
    return [field[c] - k[c] * along for c in range(3)]


def greet(rows, cols):
    row, col = lax.axis_index("row"), lax.axis_index("col")
    barrier = pltpu.get_barrier_semaphore()
    for k in range(1, cols):
        pl.semaphore_signal(
            barrier, inc=1, device_id={"col": (col + k) % cols},
            device_id_type=pl.DeviceIdType.MESH,
        )
    for k in range(1, rows):
        pl.semaphore_signal(
            barrier, inc=1, device_id={"row": (row + k) % rows},
            device_id_type=pl.DeviceIdType.MESH,
        )
    pl.semaphore_wait(barrier, rows + cols - 2)


def remote(src, dst, send, recv, axis, index):
    return pltpu.make_async_remote_copy(
        src_ref=src, dst_ref=dst, send_sem=send, recv_sem=recv,
        device_id={axis: index}, device_id_type=pl.DeviceIdType.MESH,
    )


def backward_part(
    plan, grid_in, ixh, ixl, fxh, fxl, ch, cl, sh, sl,
    modes, blocks, spans, lines, row_send, row_recv, col_send, col_recv,
):
    row, col = lax.axis_index("row"), lax.axis_index("col")
    rows, cols, by, bz, zg = plan.rows, plan.cols, plan.by, plan.bz, plan.zg
    slots, octs, nh = plan.slots, plan.octs, plan.nh
    chunks = nh * 5

    def grid_step(g, carry):
        fields = []
        for c in range(3):
            lines_z = [
                grid_in[c, pl.ds(g * zg + z, slots, stride=plan.stride), :]
                for z in range(zg)
            ]
            packed = jnp.concatenate(
                [
                    jnp.concatenate([f[:, :by] for f in lines_z], 1),
                    jnp.concatenate([f[:, by:] for f in lines_z], 1),
                ],
                0,
            )
            high, low = split(packed)
            fields.append(dot3(ixh[...], ixl[...], high, low))
        u, v, w = fields
        ww = w * w
        for p, product in enumerate((u * u - ww, v * v - ww, u * v, u * w, v * w)):
            high, low = split(product)
            made = dot3(fxh[...], fxl[...], high, low)
            for z in range(zg):
                line = jnp.concatenate(
                    [
                        made[:slots, z * by : (z + 1) * by],
                        made[slots:, z * by : (z + 1) * by],
                    ],
                    1,
                )
                for o in range(octs):
                    blocks[
                        p, o, pl.ds(pl.multiple_of((g * zg + z) * OCT, OCT), OCT), :
                    ] = line[o * OCT : (o + 1) * OCT]
        return carry

    lax.fori_loop(0, bz // zg, grid_step, 0)

    def row_copy(c, o, s, source):
        return remote(
            blocks.at[c % 5, o],
            spans.at[c, pl.ds(source * bz * OCT, bz * OCT), :],
            row_send.at[c, s], row_recv.at[c, source], "row", s,
        )

    def live(s, c):
        return s * nh + c // 5 < octs

    def send(c, carry):
        for j in range(1, rows):
            s = (row + j) % rows

            @pl.when(live(s, c))
            def _():
                row_copy(c, s * nh + c // 5, s, row).start()

        return carry

    lax.fori_loop(0, AHEAD, send, 0)

    def col_copy(c, q, source):
        low, n = plan.window[q]
        off = plan.offset[q]
        return remote(
            lines.at[c, :, pl.ds(off, n), :],
            modes.at[c, source, :, pl.ds(low, n), :],
            col_send.at[c, q], col_recv.at[c, source], "col", q,
        )

    def keep_copy(c, q):
        low, n = plan.window[q]
        off = plan.offset[q]
        return pltpu.make_async_copy(
            lines.at[c, :, pl.ds(off, n), :],
            modes.at[c, col, :, pl.ds(low, n), :],
            col_send.at[c, q],
        )

    def span_step(c, carry):
        @pl.when(jnp.logical_not(live(row, c)) & (c + AHEAD < chunks))
        def _():
            send(c + AHEAD, 0)

        @pl.when(live(row, c))
        def _():
            spans[c, pl.ds(pl.multiple_of(row * bz * OCT, OCT), bz * OCT), :] = blocks[
                c % 5, row * nh + c // 5
            ]
            for j in range(1, rows):
                row_copy(c, 0, row, (row + j) % rows).wait_recv()

            @pl.when(c + AHEAD < chunks)
            def _():
                send(c + AHEAD, 0)

            for k in range(0, OCT, 2):
                x = [
                    spans[c, pl.ds(k + m, NZ, stride=OCT), :] for m in range(2)
                ]
                turned = [jnp.concatenate([f[:, by:], -f[:, :by]], 1) for f in x]
                xh, xl = split(jnp.concatenate(x, 1))
                th, tl = split(jnp.concatenate(turned, 1))
                made = dot3(ch[...], cl[...], xh, xl) + dot3(sh[...], sl[...], th, tl)
                for m in range(2):
                    lines[c, k + m] = made[:, m * 2 * by : (m + 1) * 2 * by]
            for j in range(1, cols):
                for q in range(cols):
                    if plan.window[q][1]:

                        @pl.when((col + j) % cols == q)
                        def _():
                            col_copy(c, q, col).start()

            for q in range(cols):
                if plan.window[q][1]:

                    @pl.when(col == q)
                    def _():
                        keep_copy(c, q).start()

        return carry

    lax.fori_loop(0, chunks, span_step, 0)

    def drain(c, carry):
        for j in range(1, rows):
            s = (row + j) % rows

            @pl.when(live(s, c))
            def _():
                row_copy(c, s * nh + c // 5, s, row).wait_send()

        @pl.when(live(row, c))
        def _():
            for q in range(cols):
                if plan.window[q][1]:

                    @pl.when(col == q)
                    def _():
                        keep_copy(c, q).wait()
                        for j in range(1, cols):
                            col_copy(c, q, (q + j) % cols).wait_recv()

                    @pl.when(col != q)
                    def _():
                        col_copy(c, q, col).wait_send()

        return carry

    lax.fori_loop(0, chunks, drain, 0)


def middle_kernel(
    plan, amount, real, vel, yh, yl, ch, cl, sh, sl,
    ixh, ixl, fxh, fxl, bch, bcl, bsh, bsl,
    modes, sums, grid_in, part, lines, spans, own, parts,
    col_send, col_recv, row_send, row_recv, sum_send, sum_recv, *back,
):
    step = pl.program_id(0)
    row, col = lax.axis_index("row"), lax.axis_index("col")
    rows, cols, wx, wz, by, bz = plan.rows, plan.cols, plan.wx, plan.wz, plan.by, plan.bz
    shape = (wz, NY)

    @pl.when(step == 0)
    def _():
        for c in range(3):
            for s in range(plan.live, plan.slots):
                grid_in[c, s * plan.stride : s * plan.stride + bz] = jnp.zeros(
                    (bz, 2 * by), F32
                )
        greet(rows, cols)

    def col_copy(i, h, q):
        low, n = plan.window[h]
        off = plan.offset[h]
        return remote(
            part.at[i, q, :, pl.ds(low, n), :], lines.at[i, :, pl.ds(off, n), :],
            col_send.at[i, q], col_recv.at[i, h], "col", q,
        )

    def row_copy(i, slot, r):
        return remote(
            spans.at[i, :, pl.ds(r * bz, bz), :],
            grid_in.at[:, pl.ds(slot * plan.stride, bz), :],
            row_send.at[i, r], row_recv.at[slot], "row", r,
        )

    def sum_copy(q):
        return remote(own, parts.at[col], sum_send.at[q], sum_recv.at[col], "col", q)

    @pl.when(step < wx)
    def _():
        i = step
        kx = row * wx + i
        k, ksq, inv, keep = geometry(kx, col * wz, real, shape)
        shift = amount[i]
        v = [[pltpu.roll(vel[c, p, 0], shift, 1) for p in range(2)] for c in range(3)]
        stress = v[0][0] * v[1][0] + v[0][1] * v[1][1]
        energy = sum(v[c][p] * v[c][p] for c in range(3) for p in range(2))
        own[i, 0:1] = jnp.sum(stress, axis=0, keepdims=True)
        own[i, 1:2] = jnp.sum(ksq * energy, axis=0, keepdims=True)

        @pl.when(kx < plan.live)
        def _():
            mask = jnp.where(keep, 1.0, 0.0)
            out = [project([v[c][p] for c in range(3)], k, inv) for p in range(2)]
            smooth = jnp.concatenate(
                [
                    jnp.concatenate([mask * out[0][c], mask * out[1][c]], 1)
                    for c in range(3)
                ],
                0,
            )
            high, low = split(smooth)
            made = dot3(high, low, yh[...], yl[...])
            for q in range(cols):
                for c in range(3):
                    part[i, q, c] = made[
                        c * wz : (c + 1) * wz, q * 2 * by : (q + 1) * 2 * by
                    ]
            for h in range(cols):
                if plan.window[h][1]:
                    low, n = plan.window[h]
                    off = plan.offset[h]

                    @pl.when(col == h)
                    def _():
                        lines[i, :, off : off + n, :] = part[i, h, :, low : low + n, :]
                        for j in range(1, cols):
                            q = (h + j) % cols
                            col_copy(i, h, q).start()

    @pl.when(step == wx)
    def _():
        for j in range(1, cols):
            sum_copy((col + j) % cols).start()

    @pl.when(step >= LAG)
    def _():
        i = step - LAG
        kx = row * wx + i

        @pl.when(kx < plan.live)
        def _():
            for h in range(cols):
                if plan.window[h][1]:

                    @pl.when(col != h)
                    def _():
                        col_copy(i, h, col).wait_recv()

            x = [lines[i, c] for c in range(3)]
            turned = [jnp.concatenate([-f[:, by:], f[:, :by]], 1) for f in x]
            xh, xl = split(jnp.concatenate(x, 1))
            th, tl = split(jnp.concatenate(turned, 1))
            made = dot3(ch[...], cl[...], xh, xl) + dot3(sh[...], sl[...], th, tl)
            for c in range(3):
                spans[i, c] = made[:, c * 2 * by : (c + 1) * 2 * by]
            for r in range(rows):

                @pl.when(row == r)
                def _():
                    for c in range(3):
                        grid_in[c, pl.ds(pl.multiple_of(kx * plan.stride, 8), bz)] = spans[
                            i, c, r * bz : (r + 1) * bz
                        ]

            for j in range(1, rows):
                row_copy(i, kx, (row + j) % rows).start()

    @pl.when(step == wx + LAG - 1)
    def _():
        def arrived(slot, carry):
            @pl.when(slot // wx != row)
            def _():
                row_copy(0, slot, row).wait_recv()

            return carry

        lax.fori_loop(0, plan.live, arrived, 0)
        backward_part(
            plan, grid_in, ixh, ixl, fxh, fxl, bch, bcl, bsh, bsl, modes, *back
        )

        def sent(i, carry):
            @pl.when(row * wx + i < plan.live)
            def _():
                for h in range(cols):
                    if plan.window[h][1]:

                        @pl.when(col == h)
                        def _():
                            for j in range(1, cols):
                                col_copy(i, h, (h + j) % cols).wait_send()

                for j in range(1, rows):
                    row_copy(i, row * wx + i, (row + j) % rows).wait_send()

            return carry

        lax.fori_loop(0, wx, sent, 0)
        total = own[...]
        for j in range(1, cols):
            h = (col + j) % cols
            remote(
                own, parts.at[h], sum_send.at[h], sum_recv.at[h], "col", h
            ).wait()
        parts[col] = total
        sums[...] = sum(parts[h] for h in range(cols))


def last_kernel(plan, amount, base, real, vel, acc, modes, fh, fl, new_vel, new_acc, hats):
    shape = vel.shape[3:]
    kx = base[0] + pl.program_id(0)
    k, ksq, inv, keep = geometry(kx, base[1], real, shape)
    shift = amount[pl.program_id(0)]
    viscosity, shear, step = real[0], real[1], real[3]
    coupling = 2.0 * shear * k[0] * inv
    wz = shape[0]

    @pl.when(kx < plan.live)
    def _():
        packed = jnp.concatenate(
            [
                jnp.concatenate([modes[0, p, h, 0] for h in range(plan.cols)], 1)
                for p in range(5)
            ],
            0,
        )
        high, low = split(packed)
        hats[...] = dot3(high, low, fh[...], fl[...])

    for p in range(2):
        v = [pltpu.roll(vel[c, p, 0], shift, 1) for c in range(3)]
        old = [pltpu.roll(acc[c, p, 0], shift, 1) for c in range(3)]
        other = slice((1 - p) * NY, (2 - p) * NY)
        e0, e1, e01, e02, e12 = [
            jnp.where(keep, hats[m * wz : (m + 1) * wz, other], 0.0) for m in range(5)
        ]
        sign = 1.0 if p == 0 else -1.0
        hat = [
            sign * (k[0] * e0 + k[1] * e01 + k[2] * e02),
            sign * (k[0] * e01 + k[1] * e1 + k[2] * e12),
            sign * (k[0] * e02 + k[1] * e12),
        ]
        hat = project(hat, k, inv)
        for c in range(3):
            rate = hat[c] + coupling * k[c] * v[1] - viscosity * ksq * v[c]
            if c == 0:
                rate = rate - shear * v[1]
            total = (-5.0 / 9.0) * old[c] + step * rate
            new_acc[c, p, 0] = total
            new_vel[c, p, 0] = v[c] + (15.0 / 16.0) * total


def body(velocity, accumulator, remesh_flag, remesh_shift, viscosity, shear, clock, step):
    rows = lax.axis_size("row")
    cols = lax.axis_size("col")
    _, _, wx, wz, full_y = velocity.shape
    plan = Plan(rows, cols, wx, wz)
    by, bz = plan.by, plan.bz
    table = make_tables(plan)
    amount = jnp.mod(-(remesh_flag * remesh_shift), full_y).astype(jnp.int32)
    base = jnp.stack([lax.axis_index("row") * wx, lax.axis_index("col") * wz]).astype(
        jnp.int32
    )
    real = jnp.concatenate([viscosity, shear, clock, step, shear * clock])
    whole = pl.BlockSpec(memory_space=pltpu.VMEM)
    kz = len(plan.kz)
    chunks = plan.nh * 5
    dma = pltpu.SemaphoreType.DMA
    modes, sums = pl.pallas_call(
        functools.partial(middle_kernel, plan),
        grid_spec=pltpu.PrefetchScalarGridSpec(
            num_scalar_prefetch=2,
            grid=(wx + LAG,),
            in_specs=[
                pl.BlockSpec(
                    (3, 2, 1, wz, full_y),
                    lambda i, *_: (0, 0, jnp.minimum(i, wx - 1), 0, 0),
                )
            ]
            + [whole] * 14,
            out_specs=[pl.BlockSpec(memory_space=pl.ANY), whole],
            scratch_shapes=[
                pltpu.VMEM((3, plan.slots * plan.stride, 2 * by), F32),
                pltpu.VMEM((wx, cols, 3, wz, 2 * by), F32),
                pltpu.VMEM((wx, 3, kz, 2 * by), F32),
                pltpu.VMEM((wx, 3, NZ, 2 * by), F32),
                pltpu.VMEM((wx, 2, full_y), F32),
                pltpu.VMEM((cols, wx, 2, full_y), F32),
                dma((wx, cols)),
                dma((wx, cols)),
                dma((wx, rows)),
                dma((plan.live,)),
                dma((cols,)),
                dma((cols,)),
                pltpu.VMEM((5, plan.octs, bz * OCT, 2 * by), F32),
                pltpu.VMEM((chunks, NZ * OCT, 2 * by), F32),
                pltpu.VMEM((chunks, OCT, kz, 2 * by), F32),
                dma((chunks, rows)),
                dma((chunks, rows)),
                dma((chunks, cols)),
                dma((chunks, cols)),
            ],
        ),
        out_shape=[
            jax.ShapeDtypeStruct((chunks, cols, OCT, wz, 2 * by), F32),
            jax.ShapeDtypeStruct((wx, 2, full_y), F32),
        ],
        compiler_params=pltpu.CompilerParams(
            dimension_semantics=("arbitrary",), vmem_limit_bytes=VMEM_BYTES,
            collective_id=0, has_side_effects=True,
        ),
    )(
        amount, real, velocity, *table["inv_y"], *table["inv_z"],
        *table["inv_x"], *table["fwd_x"], *table["fwd_z"],
    )
    modes = modes.reshape(plan.nh, 5, cols, OCT, wz, 2 * by)
    state_spec = pl.BlockSpec((3, 2, 1, wz, full_y), lambda i, *_: (0, 0, i, 0, 0))
    new_velocity, new_accumulator = pl.pallas_call(
        functools.partial(last_kernel, plan),
        grid_spec=pltpu.PrefetchScalarGridSpec(
            num_scalar_prefetch=3,
            grid=(wx,),
            in_specs=[state_spec] * 2
            + [
                pl.BlockSpec(
                    (1, 5, cols, 1, wz, 2 * by),
                    lambda i, *_: (i // OCT, 0, 0, i % OCT, 0, 0),
                )
            ]
            + [whole] * 2,
            out_specs=[state_spec] * 2,
            scratch_shapes=[pltpu.VMEM((5 * wz, 2 * full_y), F32)],
        ),
        out_shape=[jax.ShapeDtypeStruct(velocity.shape, F32)] * 2,
        compiler_params=pltpu.CompilerParams(
            dimension_semantics=("arbitrary",), vmem_limit_bytes=48 * 1024 * 1024
        ),
    )(amount, base, real, velocity, accumulator, modes, *table["fwd_y"])
    totals = jnp.sum(sums, axis=-1)
    stress = totals[:, 0] / (NY * NZ)
    dissipation = 2.0 * viscosity[0] * totals[:, 1] / (NY * NZ)
    return new_velocity, new_accumulator, jnp.stack([stress, dissipation])


def solution(mesh):
    state = P(None, None, "row", "col", None)
    in_specs = (state, state, P("row"), P("row"), P(), P(), P(), P())
    out_specs = (state, state, P(None, "row"))
    return jax.shard_map(
        body, mesh=mesh, in_specs=in_specs, out_specs=out_specs, check_vma=False
    )
```

```python
import functools

import jax
import jax.numpy as jnp
import ml_dtypes
import numpy as np
from jax import lax
from jax.experimental import pallas as pl
from jax.experimental.pallas import tpu as pltpu
from jax.sharding import PartitionSpec as P

NX = 256
NY = 256
NZ = 256
LAG = 2
AHEAD = 2
DEPTH = 4
SLABS = 8
OCT = 8
VMEM_BYTES = 63 * 1024 * 1024
F32 = jnp.float32
BF16 = jnp.bfloat16


def tables(period):
    positions = np.arange(period)
    angles = (positions[:, None] * positions[None, :] % period) * (2.0 * np.pi / period)
    factor = 1.0 / np.sqrt(period)
    return np.cos(angles) * factor, np.sin(angles) * factor


def halves(table):
    table = np.ascontiguousarray(table).astype(np.float32)
    high = table.astype(ml_dtypes.bfloat16)
    low = (table - high.astype(np.float32)).astype(ml_dtypes.bfloat16)
    return [jnp.asarray(high), jnp.asarray(low)]


class Plan:
    def __init__(self, rows, cols, width_x, width_z):
        self.rows, self.cols = rows, cols
        self.wx, self.wz = width_x, width_z
        self.by, self.bz = NY // cols, NZ // rows
        self.live = sum(1 for k in range(rows * width_x) if 3 * k < NX)
        self.slots = -(-self.live // OCT) * OCT
        self.half = cols // 2
        alive = [3 * min(k, NZ - k) < NZ for k in range(NZ)]
        self.window = []
        self.offset = []
        total = 0
        for h in range(cols):
            inside = [k for k in range(width_z) if alive[h * width_z + k]]
            low = inside[0] // 8 * 8 if inside else 0
            high = -(-(inside[-1] + 1) // 8) * 8 if inside else 0
            self.window.append((low, high - low))
            self.offset.append(total)
            total += high - low
        self.kz = [
            h * width_z + low + k for h, (low, n) in enumerate(self.window) for k in range(n)
        ]
        self.side_rows = total // 2
        assert cols % 2 == 0 and self.offset[self.half] * 2 == total
        ky = [j if 2 * j < NY else j - NY for j in range(NY)]
        self.ky = [j for j in range(NY) if 3 * abs(ky[j]) < NY]
        self.ky_live = len(self.ky)
        self.lanes = 384
        self.stride = self.bz + 8 if self.bz % 16 == 0 else self.bz
        self.zg = max(1, min(self.bz, 256 // self.by))


def make_tables(plan):
    cos_x, sin_x = tables(NX)
    cos_y, sin_y = tables(NY)
    cos_z, sin_z = tables(NZ)
    cy = cos_y.reshape(NY, plan.cols, plan.by)
    sy = sin_y.reshape(NY, plan.cols, plan.by)
    inv_y = np.concatenate(
        [np.concatenate([cy, sy], 2), np.concatenate([-sy, cy], 2)], 0
    ).reshape(2 * NY, 2 * NY)
    inv_zc, inv_zs = cos_z[:, plan.kz], sin_z[:, plan.kz]
    kx = np.arange(plan.slots)
    weight = np.where(kx == 0, 1.0, 2.0) * (kx < plan.live)
    cx, sx = cos_x[:, : plan.slots], sin_x[:, : plan.slots]
    inv_x = np.concatenate([cx * weight, -sx * weight], 1)
    keep = (kx < plan.live)[:, None]
    fwd_x = np.concatenate([cx.T * keep, -sx.T * keep], 0)
    pad = [(0, 0), (0, 192 - plan.ky_live)]
    cy, sy = np.pad(cos_y[:, plan.ky], pad), np.pad(sin_y[:, plan.ky], pad)

    def lanes(re, im):
        return np.concatenate([re[:, :128], im[:, :128], re[:, 128:], im[:, 128:]], 1)

    block = []
    for h in range(plan.cols):
        y = slice(h * plan.by, (h + 1) * plan.by)
        block.append(np.concatenate([lanes(cy[y], -sy[y]), lanes(sy[y], cy[y])], 0))
    side_y = np.stack(
        [
            np.concatenate(
                [block[h // plan.half * plan.half + (h + j) % plan.half] for j in range(plan.half)], 0
            )
            for h in range(plan.cols)
        ]
    )
    signed = np.array([j if 2 * j < NY else j - NY for j in plan.ky], np.float64)
    signed = np.pad(signed, (0, 192 - plan.ky_live))[None]
    ky = np.repeat(lanes(signed, signed), 8, 0)
    kz = np.array([j if 2 * j < NZ else j - NZ for j in plan.kz], np.float64)
    kz = np.repeat(kz.reshape(2, plan.side_rows, 1)[::-1], plan.lanes, 2)
    return {
        "inv_y": halves(inv_y),
        "inv_z": halves(inv_zc) + halves(inv_zs),
        "inv_x": halves(inv_x),
        "fwd_x": halves(fwd_x),
        "fwd_z": halves(inv_zc.T) + halves(inv_zs.T),
        "side_y": halves(side_y),
        "ky": jnp.asarray(ky, F32),
        "kz_far": jnp.asarray(np.ascontiguousarray(kz), F32),
    }


def split(value):
    high = value.astype(BF16)
    return high, (value - high.astype(F32)).astype(BF16)


def mul(a, b):
    return jnp.dot(a, b, preferred_element_type=F32)


def dot3(ah, al, bh, bl):
    return mul(ah, bh) + mul(ah, bl) + mul(al, bh)


def geometry(kx, first_z, real, shape):
    iz = lax.broadcasted_iota(jnp.int32, shape, 0) + first_z
    iz = jnp.where(2 * iz < NZ, iz, iz - NZ)
    iy = lax.broadcasted_iota(jnp.int32, shape, 1)
    iy = jnp.where(2 * iy < NY, iy, iy - NY)
    k0 = jnp.full(shape, kx.astype(F32), F32)
    k1 = iy.astype(F32) - real[4] * k0
    k2 = iz.astype(F32)
    ksq = k0 * k0 + k1 * k1 + k2 * k2
    inv = 1.0 / jnp.maximum(ksq, 1.0)
    keep = (3 * jnp.abs(iz) < NZ) & (3 * jnp.abs(iy) < NY) & (3.0 * k0 < float(NX))
    return (k0, k1, k2), ksq, inv, keep


def project(field, k, inv):
    along = (k[0] * field[0] + k[1] * field[1] + k[2] * field[2]) * inv
    return [field[c] - k[c] * along for c in range(3)]


def greet(rows, cols):
    row, col = lax.axis_index("row"), lax.axis_index("col")
    barrier = pltpu.get_barrier_semaphore()
    for k in range(1, cols):
        pl.semaphore_signal(
            barrier, inc=1, device_id={"col": (col + k) % cols},
            device_id_type=pl.DeviceIdType.MESH,
        )
    for k in range(1, rows):
        pl.semaphore_signal(
            barrier, inc=1, device_id={"row": (row + k) % rows},
            device_id_type=pl.DeviceIdType.MESH,
        )
    pl.semaphore_wait(barrier, rows + cols - 2)


def remote(src, dst, send, recv, axis, index):
    return pltpu.make_async_remote_copy(
        src_ref=src, dst_ref=dst, send_sem=send, recv_sem=recv,
        device_id={axis: index}, device_id_type=pl.DeviceIdType.MESH,
    )


def reduce_modes(t, k0, k1, k2):
    t0, t1, t01, t02, t12 = t
    d0 = k0 * t0 + k1 * t01 + k2 * t02
    d1 = k0 * t01 + k1 * t1 + k2 * t12
    d2 = k0 * t02 + k1 * t12
    h2 = k0 * k0 + k2 * k2
    flat = h2 == 0.0
    first = jnp.where(flat, d0, k2 * d0 - k0 * d2)
    second = jnp.where(flat, d2, k1 * (k0 * d0 + k2 * d2) - h2 * d1)
    return first, second


def backward_part(
    plan, real, grid_in, ixh, ixl, fxh, fxl, ch, cl, sh, sl, yh, yl, ky, kz_far,
    out, blocks, spans, lines, near, relay, pairs, far,
    row_send, row_recv, near_send, near_recv, relay_send, relay_recv, far_send, far_recv,
):
    row, col = lax.axis_index("row"), lax.axis_index("col")
    rows, cols, by, bz, zg = plan.rows, plan.cols, plan.by, plan.bz, plan.zg
    wx, wz, slots, half, ns = plan.wx, plan.wz, plan.slots, plan.half, plan.side_rows
    side = col // half
    local = col % half
    other = 1 - side
    gate = jnp.where(side == 0, half - 1, half)
    far_gate = jnp.where(side == 0, half, half - 1)
    far_first = other * ns
    lk = ky.shape[1]

    def grid_step(g, carry):
        fields = []
        for c in range(3):
            lines_z = [
                grid_in[c, pl.ds(g * zg + z, slots, stride=plan.stride), :]
                for z in range(zg)
            ]
            packed = jnp.concatenate(
                [
                    jnp.concatenate([f[:, :by] for f in lines_z], 1),
                    jnp.concatenate([f[:, by:] for f in lines_z], 1),
                ],
                0,
            )
            high, low = split(packed)
            fields.append(dot3(ixh[...], ixl[...], high, low))
        u, v, w = fields
        ww = w * w
        for p, product in enumerate((u * u - ww, v * v - ww, u * v, u * w, v * w)):
            high, low = split(product)
            made = dot3(fxh[...], fxl[...], high, low)
            for z in range(zg):
                blocks[p, pl.ds(g * zg + z, slots, stride=plan.stride), :] = (
                    jnp.concatenate(
                        [
                            made[:slots, z * by : (z + 1) * by],
                            made[slots:, z * by : (z + 1) * by],
                        ],
                        1,
                    )
                )
        return carry

    lax.fori_loop(0, bz // zg, grid_step, 0)

    def row_copy(i, s, source):
        return remote(
            blocks.at[:, pl.ds((s * wx + i) * plan.stride, bz), :],
            spans.at[i, :, pl.ds(source * bz, bz), :],
            row_send.at[i % DEPTH, s], row_recv.at[i, source], "row", s,
        )

    def live(s, i):
        return s * wx + i < plan.live

    def row_wait(i):
        for j in range(1, rows):
            s = (row + j) % rows

            @pl.when(live(s, i))
            def _():
                row_copy(i, s, row).wait_send()

    def row_start(i):
        @pl.when(i >= DEPTH)
        def _():
            row_wait(i - DEPTH)

        for j in range(1, rows):
            s = (row + j) % rows

            @pl.when(live(s, i))
            def _():
                row_copy(i, s, row).start()

    for i in range(AHEAD):
        row_start(i)

    def near_copy(i, q, slot, mine):
        low, n = plan.window[q]
        return remote(
            lines.at[i % DEPTH, :, pl.ds(plan.offset[q], n), :],
            near.at[i, slot, :, pl.ds(low, n), :],
            near_send.at[i % DEPTH, slot], near_recv.at[i, slot], "col", mine,
        )

    def relay_copy(i, slot):
        return remote(
            lines.at[i % DEPTH, :, pl.ds(pl.multiple_of(far_first, 8), ns), :],
            relay.at[i, slot], relay_send.at[i % DEPTH], relay_recv.at[i, slot],
            "col", gate,
        )

    def far_copy(i, q, target):
        low, n = plan.window[q]
        first = plan.offset[q] - q // half * ns
        return remote(
            pairs.at[i % DEPTH, :, pl.ds(first, n), :],
            far.at[i, :, pl.ds(low, n), :],
            far_send.at[i % DEPTH, q], far_recv.at[i], "col", target,
        )

    def each_near(act):
        for j in range(1, half):
            q = side * half + (local + j) % half
            for h in range(cols):
                if plan.window[h][1]:

                    @pl.when(q == h)
                    def _():
                        act(h, half - j)

    def each_far(act):
        for h in range(cols):
            if plan.window[h][1]:

                @pl.when((col == gate) & (h // half == other))
                def _():
                    act(h)

    def wait_lines(i):
        each_near(lambda h, slot: near_copy(i, h, slot, h).wait_send())

        @pl.when(col != gate)
        def _():
            relay_copy(i, 1).wait_send()

    def wait_pairs(i):
        each_far(lambda h: far_copy(i, h, h).wait_send())

    def lines_step(i):
        spans[i, :, pl.ds(pl.multiple_of(row * bz, 8), bz), :] = blocks[
            :, pl.ds(pl.multiple_of((row * wx + i) * plan.stride, 8), bz), :
        ]
        for j in range(1, rows):
            row_copy(i, row, (row + j) % rows).wait_recv()

        @pl.when(i + AHEAD < wx)
        def _():
            row_start(i + AHEAD)

        @pl.when(i >= DEPTH)
        def _():
            wait_lines(i - DEPTH)

        x = [spans[i, p] for p in range(5)]
        turned = [jnp.concatenate([f[:, by:], -f[:, :by]], 1) for f in x]
        xh, xl = split(jnp.concatenate(x, 1))
        th, tl = split(jnp.concatenate(turned, 1))
        made = dot3(ch[...], cl[...], xh, xl) + dot3(sh[...], sl[...], th, tl)
        for p in range(5):
            lines[i % DEPTH, p] = made[:, p * 2 * by : (p + 1) * 2 * by]
        each_near(lambda h, slot: near_copy(i, h, slot, h).start())
        for j in range(1, half):

            @pl.when((local + j) % half == gate % half)
            def _():
                relay_copy(i, half - j).start()

        for h in range(cols):
            if plan.window[h][1]:
                low, n = plan.window[h]
                off = plan.offset[h]

                @pl.when(col == h)
                def _():
                    near[i, 0, :, low : low + n, :] = lines[
                        i % DEPTH, :, off : off + n, :
                    ]

    def transform(pieces, rows_in):
        high, low = split(jnp.concatenate([g.reshape(5 * rows_in, 2 * by) for g in pieces], 1))
        made = dot3(high, low, yh[...], yl[...])
        return [made[p * rows_in : (p + 1) * rows_in] for p in range(5)]

    def wave(i):
        k0 = jnp.full((1, lk), (row * wx + i).astype(F32), F32)
        return k0, ky[0:1] - real[4] * k0

    def relay_step(i):
        @pl.when(col == gate)
        def _():
            for j in range(1, half):
                relay_copy(i, j).wait_recv()

            @pl.when(i >= DEPTH)
            def _():
                wait_pairs(i - DEPTH)

            mine = lines[i % DEPTH, :, pl.ds(pl.multiple_of(far_first, 8), ns), :]
            t = transform([mine] + [relay[i, j] for j in range(1, half)], ns)
            k0, k1 = wave(i)
            first, second = reduce_modes(t, k0, k1, kz_far[...])
            pairs[i % DEPTH, 0] = first
            pairs[i % DEPTH, 1] = second
            each_far(lambda h: far_copy(i, h, h).start())

    def out_step(i):
        for h in range(cols):
            if plan.window[h][1]:

                @pl.when(col == h)
                def _():
                    for j in range(1, half):
                        near_copy(i, h, j, h).wait_recv()

        t = transform([near[i, j] for j in range(half)], wz)
        k0, k1 = wave(i)
        iz = lax.broadcasted_iota(jnp.int32, (wz, lk), 0) + col * wz
        k2 = jnp.where(2 * iz < NZ, iz, iz - NZ).astype(F32)
        first, second = reduce_modes(t, k0, k1, k2)
        for h in range(cols):
            if plan.window[h][1]:

                @pl.when(col == h)
                def _():
                    far_copy(i, h, far_gate).wait_recv()

        out[i, 0] = first + far[i, 0]
        out[i, 1] = second + far[i, 1]

    def span_step(t, carry):
        @pl.when((t + AHEAD < wx) & jnp.logical_not(live(row, t)))
        def _():
            row_start(t + AHEAD)

        @pl.when((t < wx) & live(row, t))
        def _():
            lines_step(t)

        @pl.when((t >= 1) & (t < wx + 1) & live(row, t - 1))
        def _():
            relay_step(t - 1)

        @pl.when((t >= 2) & live(row, t - 2))
        def _():
            out_step(t - 2)

        return carry

    lax.fori_loop(0, wx + 2, span_step, 0)

    def drain(i, carry):
        row_wait(i)
        return carry

    lax.fori_loop(wx - DEPTH, wx, drain, 0)

    def drain_lines(i, carry):
        @pl.when(live(row, i) & jnp.logical_not((i + DEPTH < wx) & live(row, i + DEPTH)))
        def _():
            wait_lines(i)
            wait_pairs(i)

        return carry

    lax.fori_loop(0, wx, drain_lines, 0)


def middle_kernel(
    plan, amount, real, vel, yh, yl, ch, cl, sh, sl,
    ixh, ixl, fxh, fxl, bch, bcl, bsh, bsl, byh, byl, ky, kz_far,
    out, sums, grid_in, part, lines, spans, own, parts,
    col_send, col_recv, row_send, row_recv, sum_send, sum_recv, *back,
):
    step = pl.program_id(0)
    row, col = lax.axis_index("row"), lax.axis_index("col")
    rows, cols, wx, wz, by, bz = plan.rows, plan.cols, plan.wx, plan.wz, plan.by, plan.bz
    shape = (wz, NY)

    @pl.when(step == 0)
    def _():
        for c in range(3):
            for s in range(plan.live, plan.slots):
                grid_in[c, s * plan.stride : s * plan.stride + bz] = jnp.zeros(
                    (bz, 2 * by), F32
                )
        greet(rows, cols)

    def col_copy(i, h, q):
        low, n = plan.window[h]
        off = plan.offset[h]
        return remote(
            part.at[i % SLABS, q, :, pl.ds(low, n), :], lines.at[i, :, pl.ds(off, n), :],
            col_send.at[i % SLABS, q], col_recv.at[i, h], "col", q,
        )

    def row_copy(i, slot, r):
        return remote(
            spans.at[i % DEPTH, :, pl.ds(r * bz, bz), :],
            grid_in.at[:, pl.ds(slot * plan.stride, bz), :],
            row_send.at[i % DEPTH, r], row_recv.at[slot], "row", r,
        )

    def sum_copy(q):
        return remote(own, parts.at[col], sum_send.at[q], sum_recv.at[col], "col", q)

    def wait_part(i):
        for h in range(cols):
            if plan.window[h][1]:

                @pl.when(col == h)
                def _():
                    for j in range(1, cols):
                        col_copy(i, h, (h + j) % cols).wait_send()

    def wait_spans(i):
        for j in range(1, rows):
            row_copy(i, row * wx + i, (row + j) % rows).wait_send()

    @pl.when(step < wx)
    def _():
        i = step
        kx = row * wx + i
        k, ksq, inv, keep = geometry(kx, col * wz, real, shape)
        shift = amount[i]
        v = [[pltpu.roll(vel[c, p, 0], shift, 1) for p in range(2)] for c in range(3)]
        stress = v[0][0] * v[1][0] + v[0][1] * v[1][1]
        energy = sum(v[c][p] * v[c][p] for c in range(3) for p in range(2))
        own[i, 0:1] = jnp.sum(stress, axis=0, keepdims=True)
        own[i, 1:2] = jnp.sum(ksq * energy, axis=0, keepdims=True)

        @pl.when(kx < plan.live)
        def _():
            mask = jnp.where(keep, 1.0, 0.0)
            flow = [project([v[c][p] for c in range(3)], k, inv) for p in range(2)]
            smooth = jnp.concatenate(
                [
                    jnp.concatenate([mask * flow[0][c], mask * flow[1][c]], 1)
                    for c in range(3)
                ],
                0,
            )
            high, low = split(smooth)
            made = dot3(high, low, yh[...], yl[...])

            @pl.when(i >= SLABS)
            def _():
                wait_part(i - SLABS)

            for q in range(cols):
                for c in range(3):
                    part[i % SLABS, q, c] = made[
                        c * wz : (c + 1) * wz, q * 2 * by : (q + 1) * 2 * by
                    ]
            for h in range(cols):
                if plan.window[h][1]:
                    low, n = plan.window[h]
                    off = plan.offset[h]

                    @pl.when(col == h)
                    def _():
                        lines[i, :, off : off + n, :] = part[
                            i % SLABS, h, :, low : low + n, :
                        ]
                        for j in range(1, cols):
                            col_copy(i, h, (h + j) % cols).start()

    @pl.when(step == wx)
    def _():
        for j in range(1, cols):
            sum_copy((col + j) % cols).start()

    @pl.when(step >= LAG)
    def _():
        i = step - LAG
        kx = row * wx + i

        @pl.when(kx < plan.live)
        def _():
            for h in range(cols):
                if plan.window[h][1]:

                    @pl.when(col != h)
                    def _():
                        col_copy(i, h, col).wait_recv()

            x = [lines[i, c] for c in range(3)]
            turned = [jnp.concatenate([-f[:, by:], f[:, :by]], 1) for f in x]
            xh, xl = split(jnp.concatenate(x, 1))
            th, tl = split(jnp.concatenate(turned, 1))
            made = dot3(ch[...], cl[...], xh, xl) + dot3(sh[...], sl[...], th, tl)

            @pl.when(i >= DEPTH)
            def _():
                wait_spans(i - DEPTH)

            for c in range(3):
                spans[i % DEPTH, c] = made[:, c * 2 * by : (c + 1) * 2 * by]
            grid_in[:, pl.ds(pl.multiple_of(kx * plan.stride, 8), bz), :] = spans[
                i % DEPTH, :, pl.ds(pl.multiple_of(row * bz, 8), bz), :
            ]
            for j in range(1, rows):
                row_copy(i, kx, (row + j) % rows).start()

    @pl.when(step == wx + LAG - 1)
    def _():
        def arrived(slot, carry):
            @pl.when(slot // wx != row)
            def _():
                row_copy(0, slot, row).wait_recv()

            return carry

        lax.fori_loop(0, plan.live, arrived, 0)
        backward_part(
            plan, real, grid_in, ixh, ixl, fxh, fxl, bch, bcl, bsh, bsl, byh, byl, ky,
            kz_far, out, *back
        )

        def sent(i, carry):
            def ends(depth):
                later = (i + depth < wx) & (row * wx + i + depth < plan.live)
                return (row * wx + i < plan.live) & jnp.logical_not(later)

            @pl.when(ends(SLABS))
            def _():
                wait_part(i)

            @pl.when(ends(DEPTH))
            def _():
                wait_spans(i)

            return carry

        lax.fori_loop(0, wx, sent, 0)
        total = own[...]
        for j in range(1, cols):
            h = (col + j) % cols
            remote(
                own, parts.at[h], sum_send.at[h], sum_recv.at[h], "col", h
            ).wait()
        parts[col] = total
        sums[...] = sum(parts[h] for h in range(cols))


def spread(pair, plan):
    ends = pair[:, 256:384]
    lane = lax.broadcasted_iota(jnp.int32, (pair.shape[0], NY), 1)
    rows = []
    for p in range(2):
        tail = ends if p == 0 else pltpu.roll(ends, 64, 1)
        packed = jnp.concatenate([pair[:, p * 128 : (p + 1) * 128], tail], 1)
        moved = pltpu.roll(packed, NY - plan.ky_live, 1)
        rows.append(jnp.where(2 * lane < NY, packed, moved))
    return rows


def last_kernel(plan, amount, base, real, vel, acc, modes, new_vel, new_acc):
    shape = vel.shape[3:]
    kx = base[0] + pl.program_id(0)
    k, ksq, inv, keep = geometry(kx, base[1], real, shape)
    shift = amount[pl.program_id(0)]
    viscosity, shear, step = real[0], real[1], real[3]
    coupling = 2.0 * shear * k[0] * inv
    h2 = k[0] * k[0] + k[2] * k[2]
    flat = h2 == 0.0
    ih2 = 1.0 / jnp.maximum(h2, 1.0)
    firsts = spread(modes[0, 0], plan)
    seconds = spread(modes[0, 1], plan)
    for p in range(2):
        v = [pltpu.roll(vel[c, p, 0], shift, 1) for c in range(3)]
        old = [pltpu.roll(acc[c, p, 0], shift, 1) for c in range(3)]
        sign = 1.0 if p == 0 else -1.0
        a = jnp.where(keep, sign * firsts[1 - p], 0.0)
        b = jnp.where(keep, sign * seconds[1 - p], 0.0)
        a1 = a * ih2
        b1 = b * inv
        b2 = k[1] * b1 * ih2
        hat = [
            jnp.where(flat, a, k[2] * a1 + k[0] * b2),
            jnp.where(flat, 0.0, -b1),
            jnp.where(flat, b, k[2] * b2 - k[0] * a1),
        ]
        for c in range(3):
            rate = hat[c] + coupling * k[c] * v[1] - viscosity * ksq * v[c]
            if c == 0:
                rate = rate - shear * v[1]
            total = (-5.0 / 9.0) * old[c] + step * rate
            new_acc[c, p, 0] = total
            new_vel[c, p, 0] = v[c] + (15.0 / 16.0) * total


def body(velocity, accumulator, remesh_flag, remesh_shift, viscosity, shear, clock, step):
    rows = lax.axis_size("row")
    cols = lax.axis_size("col")
    _, _, wx, wz, full_y = velocity.shape
    plan = Plan(rows, cols, wx, wz)
    by, bz, half, ns, lk = plan.by, plan.bz, plan.half, plan.side_rows, plan.lanes
    table = make_tables(plan)
    amount = jnp.mod(-(remesh_flag * remesh_shift), full_y).astype(jnp.int32)
    col = lax.axis_index("col")
    base = jnp.stack([lax.axis_index("row") * wx, col * wz]).astype(jnp.int32)
    real = jnp.concatenate([viscosity, shear, clock, step, shear * clock])
    side_y = [lax.dynamic_index_in_dim(t, col, 0, False) for t in table["side_y"]]
    kz_far = lax.dynamic_index_in_dim(table["kz_far"], col // half, 0, False)
    whole = pl.BlockSpec(memory_space=pltpu.VMEM)
    kz = len(plan.kz)
    dma = pltpu.SemaphoreType.DMA
    modes, sums = pl.pallas_call(
        functools.partial(middle_kernel, plan),
        grid_spec=pltpu.PrefetchScalarGridSpec(
            num_scalar_prefetch=2,
            grid=(wx + LAG,),
            in_specs=[
                pl.BlockSpec(
                    (3, 2, 1, wz, full_y),
                    lambda i, *_: (0, 0, jnp.minimum(i, wx - 1), 0, 0),
                )
            ]
            + [whole] * 18,
            out_specs=[whole, whole],
            scratch_shapes=[
                pltpu.VMEM((3, plan.slots * plan.stride, 2 * by), F32),
                pltpu.VMEM((SLABS, cols, 3, wz, 2 * by), F32),
                pltpu.VMEM((wx, 3, kz, 2 * by), F32),
                pltpu.VMEM((DEPTH, 3, NZ, 2 * by), F32),
                pltpu.VMEM((wx, 2, full_y), F32),
                pltpu.VMEM((cols, wx, 2, full_y), F32),
                dma((SLABS, cols)),
                dma((wx, cols)),
                dma((DEPTH, rows)),
                dma((plan.live,)),
                dma((cols,)),
                dma((cols,)),
                pltpu.VMEM((5, plan.slots * plan.stride, 2 * by), F32),
                pltpu.VMEM((wx, 5, NZ, 2 * by), F32),
                pltpu.VMEM((DEPTH, 5, kz, 2 * by), F32),
                pltpu.VMEM((wx, half, 5, wz, 2 * by), F32),
                pltpu.VMEM((wx, half, 5, ns, 2 * by), F32),
                pltpu.VMEM((DEPTH, 2, ns, lk), F32),
                pltpu.VMEM((wx, 2, wz, lk), F32),
                dma((DEPTH, rows)),
                dma((wx, rows)),
                dma((DEPTH, half)),
                dma((wx, half)),
                dma((DEPTH,)),
                dma((wx, half)),
                dma((DEPTH, cols)),
                dma((wx,)),
            ],
        ),
        out_shape=[
            jax.ShapeDtypeStruct((wx, 2, wz, lk), F32),
            jax.ShapeDtypeStruct((wx, 2, full_y), F32),
        ],
        compiler_params=pltpu.CompilerParams(
            dimension_semantics=("arbitrary",), vmem_limit_bytes=VMEM_BYTES,
            collective_id=0, has_side_effects=True,
        ),
    )(
        amount, real, velocity, *table["inv_y"], *table["inv_z"],
        *table["inv_x"], *table["fwd_x"], *table["fwd_z"], *side_y, table["ky"], kz_far,
    )
    state_spec = pl.BlockSpec((3, 2, 1, wz, full_y), lambda i, *_: (0, 0, i, 0, 0))
    new_velocity, new_accumulator = pl.pallas_call(
        functools.partial(last_kernel, plan),
        grid_spec=pltpu.PrefetchScalarGridSpec(
            num_scalar_prefetch=3,
            grid=(wx,),
            in_specs=[state_spec] * 2
            + [pl.BlockSpec((1, 2, wz, lk), lambda i, *_: (i, 0, 0, 0))],
            out_specs=[state_spec] * 2,
        ),
        out_shape=[jax.ShapeDtypeStruct(velocity.shape, F32)] * 2,
        compiler_params=pltpu.CompilerParams(
            dimension_semantics=("arbitrary",), vmem_limit_bytes=48 * 1024 * 1024
        ),
    )(amount, base, real, velocity, accumulator, modes)
    totals = jnp.sum(sums, axis=-1)
    stress = totals[:, 0] / (NY * NZ)
    dissipation = 2.0 * viscosity[0] * totals[:, 1] / (NY * NZ)
    return new_velocity, new_accumulator, jnp.stack([stress, dissipation])


def solution(mesh):
    state = P(None, None, "row", "col", None)
    in_specs = (state, state, P("row"), P("row"), P(), P(), P(), P())
    out_specs = (state, state, P(None, "row"))
    return jax.shard_map(
        body, mesh=mesh, in_specs=in_specs, out_specs=out_specs, check_vma=False
    )
```

```python
import functools

import jax
import jax.numpy as jnp
import ml_dtypes
import numpy as np
from jax import lax
from jax.experimental import pallas as pl
from jax.experimental.pallas import tpu as pltpu
from jax.sharding import PartitionSpec as P

NX = 256
NY = 256
NZ = 256
LAG = 2
AHEAD = 2
GROUP = 2
DEPTH = 4
SLABS = 8
OCT = 8
VMEM_BYTES = 63 * 1024 * 1024
F32 = jnp.float32
BF16 = jnp.bfloat16


def tables(period):
    positions = np.arange(period)
    angles = (positions[:, None] * positions[None, :] % period) * (2.0 * np.pi / period)
    factor = 1.0 / np.sqrt(period)
    return np.cos(angles) * factor, np.sin(angles) * factor


def halves(table):
    table = np.ascontiguousarray(table).astype(np.float32)
    high = table.astype(ml_dtypes.bfloat16)
    low = (table - high.astype(np.float32)).astype(ml_dtypes.bfloat16)
    return [jnp.asarray(high), jnp.asarray(low)]


class Plan:
    def __init__(self, rows, cols, width_x, width_z):
        self.rows, self.cols = rows, cols
        self.wx, self.wz = width_x, width_z
        self.by, self.bz = NY // cols, NZ // rows
        self.live = sum(1 for k in range(rows * width_x) if 3 * k < NX)
        self.slots = -(-self.live // OCT) * OCT
        self.half = cols // 2
        alive = [3 * min(k, NZ - k) < NZ for k in range(NZ)]
        self.window = []
        self.offset = []
        total = 0
        for h in range(cols):
            inside = [k for k in range(width_z) if alive[h * width_z + k]]
            low = inside[0] // 8 * 8 if inside else 0
            high = -(-(inside[-1] + 1) // 8) * 8 if inside else 0
            self.window.append((low, high - low))
            self.offset.append(total)
            total += high - low
        self.kz = [
            h * width_z + low + k for h, (low, n) in enumerate(self.window) for k in range(n)
        ]
        self.side_rows = total // 2
        assert cols % 2 == 0 and self.offset[self.half] * 2 == total
        ky = [j if 2 * j < NY else j - NY for j in range(NY)]
        self.ky = [j for j in range(NY) if 3 * abs(ky[j]) < NY]
        self.ky_live = len(self.ky)
        self.lanes = 384
        self.stride = self.bz + 8 if self.bz % 16 == 0 else self.bz
        self.zg = max(1, min(self.bz, 256 // self.by))


def make_tables(plan):
    cos_x, sin_x = tables(NX)
    cos_y, sin_y = tables(NY)
    cos_z, sin_z = tables(NZ)
    cy = cos_y.reshape(NY, plan.cols, plan.by)
    sy = sin_y.reshape(NY, plan.cols, plan.by)
    inv_y = np.concatenate(
        [np.concatenate([cy, sy], 2), np.concatenate([-sy, cy], 2)], 0
    ).reshape(2 * NY, 2 * NY)
    inv_zc, inv_zs = cos_z[:, plan.kz], sin_z[:, plan.kz]
    kx = np.arange(plan.slots)
    weight = np.where(kx == 0, 1.0, 2.0) * (kx < plan.live)
    cx, sx = cos_x[:, : plan.slots], sin_x[:, : plan.slots]
    inv_x = np.concatenate([cx * weight, -sx * weight], 1)
    keep = (kx < plan.live)[:, None]
    fwd_x = np.concatenate([cx.T * keep, -sx.T * keep], 0)
    pad = [(0, 0), (0, 192 - plan.ky_live)]
    cy, sy = np.pad(cos_y[:, plan.ky], pad), np.pad(sin_y[:, plan.ky], pad)

    def lanes(re, im):
        return np.concatenate([re[:, :128], im[:, :128], re[:, 128:], im[:, 128:]], 1)

    block = []
    for h in range(plan.cols):
        y = slice(h * plan.by, (h + 1) * plan.by)
        block.append(np.concatenate([lanes(cy[y], -sy[y]), lanes(sy[y], cy[y])], 0))
    side_y = np.stack(block)
    signed = np.array([j if 2 * j < NY else j - NY for j in plan.ky], np.float64)
    signed = np.pad(signed, (0, 192 - plan.ky_live))[None]
    ky = np.repeat(lanes(signed, signed), 8, 0)
    return {
        "inv_y": halves(inv_y),
        "inv_z": halves(inv_zc) + halves(inv_zs),
        "inv_x": halves(inv_x),
        "fwd_x": halves(fwd_x),
        "fwd_z": halves(inv_zc.T) + halves(inv_zs.T),
        "side_y": halves(side_y),
        "ky": jnp.asarray(ky, F32),
    }


def split(value):
    high = value.astype(BF16)
    return high, (value - high.astype(F32)).astype(BF16)


def mul(a, b):
    return jnp.dot(a, b, preferred_element_type=F32)


def dot3(ah, al, bh, bl):
    return mul(ah, bh) + mul(ah, bl) + mul(al, bh)


def geometry(kx, first_z, real, shape):
    iz = lax.broadcasted_iota(jnp.int32, shape, 0) + first_z
    iz = jnp.where(2 * iz < NZ, iz, iz - NZ)
    iy = lax.broadcasted_iota(jnp.int32, shape, 1)
    iy = jnp.where(2 * iy < NY, iy, iy - NY)
    k0 = jnp.full(shape, kx.astype(F32), F32)
    k1 = iy.astype(F32) - real[4] * k0
    k2 = iz.astype(F32)
    ksq = k0 * k0 + k1 * k1 + k2 * k2
    inv = 1.0 / jnp.maximum(ksq, 1.0)
    keep = (3 * jnp.abs(iz) < NZ) & (3 * jnp.abs(iy) < NY) & (3.0 * k0 < float(NX))
    return (k0, k1, k2), ksq, inv, keep


def project(field, k, inv):
    along = (k[0] * field[0] + k[1] * field[1] + k[2] * field[2]) * inv
    return [field[c] - k[c] * along for c in range(3)]


def greet(rows, cols):
    row, col = lax.axis_index("row"), lax.axis_index("col")
    barrier = pltpu.get_barrier_semaphore()
    for k in range(1, cols):
        pl.semaphore_signal(
            barrier, inc=1, device_id={"col": (col + k) % cols},
            device_id_type=pl.DeviceIdType.MESH,
        )
    for k in range(1, rows):
        pl.semaphore_signal(
            barrier, inc=1, device_id={"row": (row + k) % rows},
            device_id_type=pl.DeviceIdType.MESH,
        )
    pl.semaphore_wait(barrier, rows + cols - 2)


def remote(src, dst, send, recv, axis, index):
    return pltpu.make_async_remote_copy(
        src_ref=src, dst_ref=dst, send_sem=send, recv_sem=recv,
        device_id={axis: index}, device_id_type=pl.DeviceIdType.MESH,
    )


def reduce_modes(t, k0, k1, k2):
    t0, t1, t01, t02, t12 = t
    d0 = k0 * t0 + k1 * t01 + k2 * t02
    d1 = k0 * t01 + k1 * t1 + k2 * t12
    d2 = k0 * t02 + k1 * t12
    h2 = k0 * k0 + k2 * k2
    flat = h2 == 0.0
    first = jnp.where(flat, d0, k2 * d0 - k0 * d2)
    second = jnp.where(flat, d2, k1 * (k0 * d0 + k2 * d2) - h2 * d1)
    return first, second


def backward_part(
    plan, real, grid_in, ixh, ixl, fxh, fxl, ch, cl, sh, sl, yh, yl, ky,
    out, blocks, spans, lines, near, relay, pairs, far,
    row_send, row_recv, near_send, near_recv, relay_send, relay_recv, far_send, far_recv,
):
    row, col = lax.axis_index("row"), lax.axis_index("col")
    rows, cols, by, bz, zg = plan.rows, plan.cols, plan.by, plan.bz, plan.zg
    wx, wz, slots, half, ns = plan.wx, plan.wz, plan.slots, plan.half, plan.side_rows
    side = col // half
    local = col % half
    other = 1 - side
    gate = jnp.where(side == 0, half - 1, half)
    far_gate = jnp.where(side == 0, half, half - 1)
    far_first = other * ns
    lk = ky.shape[1]

    def grid_step(g, carry):
        fields = []
        for c in range(3):
            lines_z = [
                grid_in[c, pl.ds(g * zg + z, slots, stride=plan.stride), :]
                for z in range(zg)
            ]
            packed = jnp.concatenate(
                [
                    jnp.concatenate([f[:, :by] for f in lines_z], 1),
                    jnp.concatenate([f[:, by:] for f in lines_z], 1),
                ],
                0,
            )
            high, low = split(packed)
            fields.append(dot3(ixh[...], ixl[...], high, low))
        u, v, w = fields
        ww = w * w
        for p, product in enumerate((u * u - ww, v * v - ww, u * v, u * w, v * w)):
            high, low = split(product)
            made = dot3(fxh[...], fxl[...], high, low)
            for z in range(zg):
                blocks[p, pl.ds(g * zg + z, slots, stride=plan.stride), :] = (
                    jnp.concatenate(
                        [
                            made[:slots, z * by : (z + 1) * by],
                            made[slots:, z * by : (z + 1) * by],
                        ],
                        1,
                    )
                )
        return carry

    lax.fori_loop(0, bz // zg, grid_step, 0)

    def row_copy(i, s, source):
        return remote(
            blocks.at[:, pl.ds((s * wx + i) * plan.stride, bz), :],
            spans.at[i, :, pl.ds(source * bz, bz), :],
            row_send.at[i % DEPTH, s], row_recv.at[i, source], "row", s,
        )

    def live(s, i):
        return s * wx + i < plan.live

    def row_wait(i):
        for j in range(1, rows):
            s = (row + j) % rows

            @pl.when(live(s, i))
            def _():
                row_copy(i, s, row).wait_send()

    def row_start(i):
        @pl.when(i >= DEPTH)
        def _():
            row_wait(i - DEPTH)

        for j in range(1, rows):
            s = (row + j) % rows

            @pl.when(live(s, i))
            def _():
                row_copy(i, s, row).start()

    for i in range(AHEAD):
        row_start(i)

    def near_copy(i, q, slot, mine):
        low, n = plan.window[q]
        return remote(
            lines.at[i % DEPTH, :, pl.ds(plan.offset[q], n), :],
            near.at[i, slot, :, pl.ds(low, n), :],
            near_send.at[i % DEPTH, slot], near_recv.at[i, slot], "col", mine,
        )

    def relay_copy(i, slot):
        return remote(
            lines.at[i % DEPTH, :, pl.ds(pl.multiple_of(far_first, 8), ns), :],
            relay.at[i, slot], relay_send.at[i % DEPTH], relay_recv.at[i, slot],
            "col", gate,
        )

    def far_copy(i, q, target):
        low, n = plan.window[q]
        first = plan.offset[q] - q // half * ns
        return remote(
            pairs.at[i % DEPTH, :, pl.ds(first, n), :],
            far.at[i, :, pl.ds(low, n), :],
            far_send.at[i % DEPTH, q], far_recv.at[i], "col", target,
        )

    def each_near(act):
        for j in range(1, half):
            q = side * half + (local + j) % half
            for h in range(cols):
                if plan.window[h][1]:

                    @pl.when(q == h)
                    def _():
                        act(h, half - j)

    def each_far(act):
        for h in range(cols):
            if plan.window[h][1]:

                @pl.when((col == gate) & (h // half == other))
                def _():
                    act(h)

    def wait_lines(i):
        each_near(lambda h, slot: near_copy(i, h, slot, h).wait_send())

        @pl.when(col != gate)
        def _():
            relay_copy(i, 1).wait_send()

    def wait_pairs(i):
        each_far(lambda h: far_copy(i, h, h).wait_send())

    def lines_step(i):
        spans[i, :, pl.ds(pl.multiple_of(row * bz, 8), bz), :] = blocks[
            :, pl.ds(pl.multiple_of((row * wx + i) * plan.stride, 8), bz), :
        ]
        for j in range(1, rows):
            row_copy(i, row, (row + j) % rows).wait_recv()

        @pl.when(i + AHEAD < wx)
        def _():
            row_start(i + AHEAD)

        @pl.when(i >= DEPTH)
        def _():
            wait_lines(i - DEPTH)

        x = [spans[i, p] for p in range(5)]
        turned = [jnp.concatenate([f[:, by:], -f[:, :by]], 1) for f in x]
        xh, xl = split(jnp.concatenate(x, 1))
        th, tl = split(jnp.concatenate(turned, 1))
        made = dot3(ch[...], cl[...], xh, xl) + dot3(sh[...], sl[...], th, tl)
        for p in range(5):
            lines[i % DEPTH, p] = made[:, p * 2 * by : (p + 1) * 2 * by]
        each_near(lambda h, slot: near_copy(i, h, slot, h).start())
        for j in range(1, half):

            @pl.when((local + j) % half == gate % half)
            def _():
                relay_copy(i, half - j).start()

        for h in range(cols):
            if plan.window[h][1]:
                low, n = plan.window[h]
                off = plan.offset[h]

                @pl.when(col == h)
                def _():
                    near[i, 0, :, low : low + n, :] = lines[
                        i % DEPTH, :, off : off + n, :
                    ]

    def transform(pieces, rows_in):
        high, low = split(jnp.concatenate([g.reshape(5 * rows_in, 2 * by) for g in pieces], 1))
        sources = [side * half + (local + j) % half for j in range(half)]
        table_h = jnp.concatenate([yh[q] for q in sources], 0)
        table_l = jnp.concatenate([yl[q] for q in sources], 0)
        made = dot3(high, low, table_h, table_l)
        return [made[p * rows_in : (p + 1) * rows_in] for p in range(5)]

    def wave(i):
        k0 = jnp.full((1, lk), (row * wx + i).astype(F32), F32)
        return k0, ky[0:1] - real[4] * k0

    def far_kz():
        line = lax.broadcasted_iota(jnp.int32, (ns, lk), 0)
        iz = jnp.zeros((ns, lk), jnp.int32)
        for q, (low, n) in enumerate(plan.window):
            first = plan.offset[q] - q // half * ns
            here = (line >= first) & (line < first + n) & (other == q // half)
            iz = jnp.where(here, line + (q * plan.wz + low - first), iz)
        return jnp.where(2 * iz < NZ, iz, iz - NZ).astype(F32)

    def relay_step(i):
        @pl.when(col == gate)
        def _():
            for j in range(1, half):
                relay_copy(i, j).wait_recv()

            @pl.when(i >= DEPTH)
            def _():
                wait_pairs(i - DEPTH)

            mine = lines[i % DEPTH, :, pl.ds(pl.multiple_of(far_first, 8), ns), :]
            t = transform([mine] + [relay[i, j] for j in range(1, half)], ns)
            k0, k1 = wave(i)
            first, second = reduce_modes(t, k0, k1, far_kz())
            pairs[i % DEPTH, 0] = first
            pairs[i % DEPTH, 1] = second
            each_far(lambda h: far_copy(i, h, h).start())

    def out_step(i):
        for h in range(cols):
            if plan.window[h][1]:

                @pl.when(col == h)
                def _():
                    for j in range(1, half):
                        near_copy(i, h, j, h).wait_recv()

        t = transform([near[i, j] for j in range(half)], wz)
        k0, k1 = wave(i)
        iz = lax.broadcasted_iota(jnp.int32, (wz, lk), 0) + col * wz
        k2 = jnp.where(2 * iz < NZ, iz, iz - NZ).astype(F32)
        first, second = reduce_modes(t, k0, k1, k2)
        for h in range(cols):
            if plan.window[h][1]:

                @pl.when(col == h)
                def _():
                    far_copy(i, h, far_gate).wait_recv()

        out[i, 0] = first + far[i, 0]
        out[i, 1] = second + far[i, 1]

    def span_step(t, carry):
        @pl.when((t + AHEAD < wx) & jnp.logical_not(live(row, t)))
        def _():
            row_start(t + AHEAD)

        @pl.when((t < wx) & live(row, t))
        def _():
            lines_step(t)

        @pl.when((t >= 1) & (t < wx + 1) & live(row, t - 1))
        def _():
            relay_step(t - 1)

        @pl.when((t >= 2) & live(row, t - 2))
        def _():
            out_step(t - 2)

        return carry

    lax.fori_loop(0, wx + 2, span_step, 0)

    def drain(i, carry):
        row_wait(i)
        return carry

    lax.fori_loop(wx - DEPTH, wx, drain, 0)

    def drain_lines(i, carry):
        @pl.when(live(row, i) & jnp.logical_not((i + DEPTH < wx) & live(row, i + DEPTH)))
        def _():
            wait_lines(i)
            wait_pairs(i)

        return carry

    lax.fori_loop(0, wx, drain_lines, 0)


def middle_kernel(
    plan, amount, real, vel, yh, yl, ch, cl, sh, sl,
    ixh, ixl, fxh, fxl, bch, bcl, bsh, bsl, byh, byl, ky,
    out, sums, grid_in, part, lines, spans, own, parts,
    col_send, col_recv, row_send, row_recv, sum_send, sum_recv, *back,
):
    step = pl.program_id(0)
    row, col = lax.axis_index("row"), lax.axis_index("col")
    rows, cols, wx, wz, by, bz = plan.rows, plan.cols, plan.wx, plan.wz, plan.by, plan.bz
    shape = (wz, NY)

    @pl.when(step == 0)
    def _():
        for c in range(3):
            for s in range(plan.live, plan.slots):
                grid_in[c, s * plan.stride : s * plan.stride + bz] = jnp.zeros(
                    (bz, 2 * by), F32
                )
        greet(rows, cols)

    def col_copy(i, h, q):
        low, n = plan.window[h]
        off = plan.offset[h]
        return remote(
            part.at[i % SLABS, q, :, pl.ds(low, n), :], lines.at[i, :, pl.ds(off, n), :],
            col_send.at[i % SLABS, q], col_recv.at[i, h], "col", q,
        )

    def row_copy(i, slot, r):
        return remote(
            spans.at[i % DEPTH, :, pl.ds(r * bz, bz), :],
            grid_in.at[:, pl.ds(slot * plan.stride, bz), :],
            row_send.at[i % DEPTH, r], row_recv.at[slot], "row", r,
        )

    def sum_copy(q):
        return remote(own, parts.at[col], sum_send.at[q], sum_recv.at[col], "col", q)

    def wait_part(i):
        for h in range(cols):
            if plan.window[h][1]:

                @pl.when(col == h)
                def _():
                    for j in range(1, cols):
                        col_copy(i, h, (h + j) % cols).wait_send()

    def wait_spans(i):
        for j in range(1, rows):
            row_copy(i, row * wx + i, (row + j) % rows).wait_send()

    @pl.when(step < wx)
    def _():
        i = step
        kx = row * wx + i
        k, ksq, inv, keep = geometry(kx, col * wz, real, shape)
        shift = amount[i]
        v = [[pltpu.roll(vel[c, p, 0], shift, 1) for p in range(2)] for c in range(3)]
        stress = v[0][0] * v[1][0] + v[0][1] * v[1][1]
        energy = sum(v[c][p] * v[c][p] for c in range(3) for p in range(2))
        own[i, 0:1] = jnp.sum(stress, axis=0, keepdims=True)
        own[i, 1:2] = jnp.sum(ksq * energy, axis=0, keepdims=True)

        @pl.when(kx < plan.live)
        def _():
            mask = jnp.where(keep, 1.0, 0.0)
            flow = [project([v[c][p] for c in range(3)], k, inv) for p in range(2)]
            smooth = jnp.concatenate(
                [
                    jnp.concatenate([mask * flow[0][c], mask * flow[1][c]], 1)
                    for c in range(3)
                ],
                0,
            )
            high, low = split(smooth)
            made = dot3(high, low, yh[...], yl[...])

            @pl.when(i >= SLABS)
            def _():
                wait_part(i - SLABS)

            for q in range(cols):
                for c in range(3):
                    part[i % SLABS, q, c] = made[
                        c * wz : (c + 1) * wz, q * 2 * by : (q + 1) * 2 * by
                    ]
            for h in range(cols):
                if plan.window[h][1]:
                    low, n = plan.window[h]
                    off = plan.offset[h]

                    @pl.when(col == h)
                    def _():
                        lines[i, :, off : off + n, :] = part[
                            i % SLABS, h, :, low : low + n, :
                        ]
                        for j in range(1, cols):
                            col_copy(i, h, (h + j) % cols).start()

    @pl.when(step == wx)
    def _():
        for j in range(1, cols):
            sum_copy((col + j) % cols).start()

    @pl.when(step >= LAG)
    def _():
        i = step - LAG
        kx = row * wx + i

        @pl.when(kx < plan.live)
        def _():
            for h in range(cols):
                if plan.window[h][1]:

                    @pl.when(col != h)
                    def _():
                        col_copy(i, h, col).wait_recv()

            x = [lines[i, c] for c in range(3)]
            turned = [jnp.concatenate([-f[:, by:], f[:, :by]], 1) for f in x]
            xh, xl = split(jnp.concatenate(x, 1))
            th, tl = split(jnp.concatenate(turned, 1))
            made = dot3(ch[...], cl[...], xh, xl) + dot3(sh[...], sl[...], th, tl)

            @pl.when(i >= DEPTH)
            def _():
                wait_spans(i - DEPTH)

            for c in range(3):
                spans[i % DEPTH, c] = made[:, c * 2 * by : (c + 1) * 2 * by]
            grid_in[:, pl.ds(pl.multiple_of(kx * plan.stride, 8), bz), :] = spans[
                i % DEPTH, :, pl.ds(pl.multiple_of(row * bz, 8), bz), :
            ]
            for j in range(1, rows):
                row_copy(i, kx, (row + j) % rows).start()

    @pl.when(step == wx + LAG - 1)
    def _():
        def arrived(slot, carry):
            @pl.when(slot // wx != row)
            def _():
                row_copy(0, slot, row).wait_recv()

            return carry

        lax.fori_loop(0, plan.live, arrived, 0)
        backward_part(
            plan, real, grid_in, ixh, ixl, fxh, fxl, bch, bcl, bsh, bsl, byh, byl, ky,
            out, *back
        )

        def sent(i, carry):
            def ends(depth):
                later = (i + depth < wx) & (row * wx + i + depth < plan.live)
                return (row * wx + i < plan.live) & jnp.logical_not(later)

            @pl.when(ends(SLABS))
            def _():
                wait_part(i)

            @pl.when(ends(DEPTH))
            def _():
                wait_spans(i)

            return carry

        lax.fori_loop(0, wx, sent, 0)
        total = own[...]
        for j in range(1, cols):
            h = (col + j) % cols
            remote(
                own, parts.at[h], sum_send.at[h], sum_recv.at[h], "col", h
            ).wait()
        parts[col] = total
        sums[...] = sum(parts[h] for h in range(cols))


def spread(pair, plan):
    ends = pair[:, 256:384]
    lane = lax.broadcasted_iota(jnp.int32, (pair.shape[0], NY), 1)
    rows = []
    for p in range(2):
        tail = ends if p == 0 else pltpu.roll(ends, 64, 1)
        packed = jnp.concatenate([pair[:, p * 128 : (p + 1) * 128], tail], 1)
        moved = pltpu.roll(packed, NY - plan.ky_live, 1)
        rows.append(jnp.where(2 * lane < NY, packed, moved))
    return rows


def update_row(m, plan, amount, base, real, vel, acc, modes, new_vel, new_acc):
    shape = vel.shape[3:]
    index = pl.program_id(0) * GROUP + m
    kx = base[0] + index
    k, ksq, inv, keep = geometry(kx, base[1], real, shape)
    shift = amount[index]
    viscosity, shear, step = real[0], real[1], real[3]
    coupling = 2.0 * shear * k[0] * inv
    h2 = k[0] * k[0] + k[2] * k[2]
    flat = h2 == 0.0
    ih2 = 1.0 / jnp.maximum(h2, 1.0)
    firsts = spread(modes[m, 0], plan)
    seconds = spread(modes[m, 1], plan)
    for p in range(2):
        v = [pltpu.roll(vel[c, p, m], shift, 1) for c in range(3)]
        old = [pltpu.roll(acc[c, p, m], shift, 1) for c in range(3)]
        sign = 1.0 if p == 0 else -1.0
        a = jnp.where(keep, sign * firsts[1 - p], 0.0)
        b = jnp.where(keep, sign * seconds[1 - p], 0.0)
        a1 = a * ih2
        b1 = b * inv
        b2 = k[1] * b1 * ih2
        hat = [
            jnp.where(flat, a, k[2] * a1 + k[0] * b2),
            jnp.where(flat, 0.0, -b1),
            jnp.where(flat, b, k[2] * b2 - k[0] * a1),
        ]
        for c in range(3):
            rate = hat[c] + coupling * k[c] * v[1] - viscosity * ksq * v[c]
            if c == 0:
                rate = rate - shear * v[1]
            total = (-5.0 / 9.0) * old[c] + step * rate
            new_acc[c, p, m] = total
            new_vel[c, p, m] = v[c] + (15.0 / 16.0) * total


def last_kernel(plan, *refs):
    for m in range(GROUP):
        update_row(m, plan, *refs)


def body(velocity, accumulator, remesh_flag, remesh_shift, viscosity, shear, clock, step):
    rows = lax.axis_size("row")
    cols = lax.axis_size("col")
    _, _, wx, wz, full_y = velocity.shape
    plan = Plan(rows, cols, wx, wz)
    by, bz, half, ns, lk = plan.by, plan.bz, plan.half, plan.side_rows, plan.lanes
    table = make_tables(plan)
    amount = jnp.mod(-(remesh_flag * remesh_shift), full_y).astype(jnp.int32)
    col = lax.axis_index("col")
    base = jnp.stack([lax.axis_index("row") * wx, col * wz]).astype(jnp.int32)
    real = jnp.concatenate([viscosity, shear, clock, step, shear * clock])
    whole = pl.BlockSpec(memory_space=pltpu.VMEM)
    kz = len(plan.kz)
    dma = pltpu.SemaphoreType.DMA
    modes, sums = pl.pallas_call(
        functools.partial(middle_kernel, plan),
        grid_spec=pltpu.PrefetchScalarGridSpec(
            num_scalar_prefetch=2,
            grid=(wx + LAG,),
            in_specs=[
                pl.BlockSpec(
                    (3, 2, 1, wz, full_y),
                    lambda i, *_: (0, 0, jnp.minimum(i, wx - 1), 0, 0),
                )
            ]
            + [whole] * 17,
            out_specs=[whole, whole],
            scratch_shapes=[
                pltpu.VMEM((3, plan.slots * plan.stride, 2 * by), F32),
                pltpu.VMEM((SLABS, cols, 3, wz, 2 * by), F32),
                pltpu.VMEM((wx, 3, kz, 2 * by), F32),
                pltpu.VMEM((DEPTH, 3, NZ, 2 * by), F32),
                pltpu.VMEM((wx, 2, full_y), F32),
                pltpu.VMEM((cols, wx, 2, full_y), F32),
                dma((SLABS, cols)),
                dma((wx, cols)),
                dma((DEPTH, rows)),
                dma((plan.live,)),
                dma((cols,)),
                dma((cols,)),
                pltpu.VMEM((5, plan.slots * plan.stride, 2 * by), F32),
                pltpu.VMEM((wx, 5, NZ, 2 * by), F32),
                pltpu.VMEM((DEPTH, 5, kz, 2 * by), F32),
                pltpu.VMEM((wx, half, 5, wz, 2 * by), F32),
                pltpu.VMEM((wx, half, 5, ns, 2 * by), F32),
                pltpu.VMEM((DEPTH, 2, ns, lk), F32),
                pltpu.VMEM((wx, 2, wz, lk), F32),
                dma((DEPTH, rows)),
                dma((wx, rows)),
                dma((DEPTH, half)),
                dma((wx, half)),
                dma((DEPTH,)),
                dma((wx, half)),
                dma((DEPTH, cols)),
                dma((wx,)),
            ],
        ),
        out_shape=[
            jax.ShapeDtypeStruct((wx, 2, wz, lk), F32),
            jax.ShapeDtypeStruct((wx, 2, full_y), F32),
        ],
        compiler_params=pltpu.CompilerParams(
            dimension_semantics=("arbitrary",), vmem_limit_bytes=VMEM_BYTES,
            collective_id=0, has_side_effects=True,
        ),
    )(
        amount, real, velocity, *table["inv_y"], *table["inv_z"],
        *table["inv_x"], *table["fwd_x"], *table["fwd_z"], *table["side_y"], table["ky"],
    )
    state_spec = pl.BlockSpec((3, 2, GROUP, wz, full_y), lambda i, *_: (0, 0, i, 0, 0))
    new_velocity, new_accumulator = pl.pallas_call(
        functools.partial(last_kernel, plan),
        grid_spec=pltpu.PrefetchScalarGridSpec(
            num_scalar_prefetch=3,
            grid=(wx // GROUP,),
            in_specs=[state_spec] * 2
            + [pl.BlockSpec((GROUP, 2, wz, lk), lambda i, *_: (i, 0, 0, 0))],
            out_specs=[state_spec] * 2,
        ),
        out_shape=[jax.ShapeDtypeStruct(velocity.shape, F32)] * 2,
        compiler_params=pltpu.CompilerParams(
            dimension_semantics=("arbitrary",), vmem_limit_bytes=VMEM_BYTES
        ),
    )(amount, base, real, velocity, accumulator, modes)
    totals = jnp.sum(sums, axis=-1)
    stress = totals[:, 0] / (NY * NZ)
    dissipation = 2.0 * viscosity[0] * totals[:, 1] / (NY * NZ)
    return new_velocity, new_accumulator, jnp.stack([stress, dissipation])


def solution(mesh):
    state = P(None, None, "row", "col", None)
    in_specs = (state, state, P("row"), P("row"), P(), P(), P(), P())
    out_specs = (state, state, P(None, "row"))
    return jax.shard_map(
        body, mesh=mesh, in_specs=in_specs, out_specs=out_specs, check_vma=False
    )
```
